8 devices in a mesh: dp: 2 (over z, y), tp: 4 (over x, core).
Axes of the slice: x: 2, y: 2, z: 1, core: 2. Of those that a mesh axis runs over, the one named last changes fastest.
Arguments:
- x_seq: bfloat16 [4, 1024, 6144], P('dp', 'tp'), parts along dimension 0
- ln_gain: bfloat16 [6144], replicated
- w_qkv: bfloat16 [6144, 8, 1024], P(None, 'tp')
- w_out: bfloat16 [6144, 6144], P('tp')
- y_grad: bfloat16 [4, 1024, 6144], P('dp', 'tp'), parts along dimension 0
Outputs:
- output 1: bfloat16 [4, 1024, 6144], P('dp', 'tp'), parts along dimension 0
- output 2: bfloat16 [4, 1024, 6144], P('dp', 'tp'), parts along dimension 0
- output 3: bfloat16 [12288], P('dp'), parts along dimension 0
- output 4: bfloat16 [12288, 8, 1024], P('dp', 'tp'), parts along dimension 0
- output 5: bfloat16 [12288, 6144], P(('dp', 'tp')), parts along dimension 0
There are 2 independent parts. The reference program is written for one: setup_inputs(seed, part) draws one part's arguments, and reference() takes and returns one part's arrays. A program takes and returns all parts, laid end to end along the dimension named above; an argument that names none is the same for every part.
All inputs are finite; a program needn't handle non-finite values.
Results may differ from the reference program's by a relative error of at most 0.0162463.
Values are sent between devices in bfloat16 or wider.
A program may use at most 1 GiB of HBM per device.

```python
import jax
import jax.numpy as jnp
from jax import lax

BATCH_SIZE = 2
SEQ_LEN = 1024
D_MODEL = 6144
N_HEADS = 48
KV_HEADS = 8
HEAD_DIM = 128
CLIP_QKV = 8
ROPE_THETA = 500000
LN_EPS = 1e-5
GROUP_SIZE = N_HEADS // KV_HEADS
SLOT_WIDTH = (GROUP_SIZE + 2) * HEAD_DIM
OUT_GAIN = max(1.0, SEQ_LEN / 256.0) ** 0.25


def setup_inputs(seed: int = 0, part: int = 0) -> dict:
    root_key = jax.random.key(seed)
    k_gain, k_qkv, k_out = jax.random.split(root_key, 3)
    k_x, k_dy = jax.random.split(jax.random.fold_in(root_key, part), 2)
    x_seq = jax.random.normal(k_x, (BATCH_SIZE, SEQ_LEN, D_MODEL), jnp.float32)
    ln_gain = 1.0 + 0.3 * jax.random.normal(k_gain, (D_MODEL,), jnp.float32)
    slot_gain = jnp.concatenate([jnp.full((GROUP_SIZE,), 5.0, dtype=jnp.float32), jnp.array([0.35, 5.0], dtype=jnp.float32)])
    w_qkv = jax.random.normal(k_qkv, (D_MODEL, KV_HEADS, GROUP_SIZE + 2, HEAD_DIM), jnp.float32)
    w_qkv = w_qkv * slot_gain[:, None] * D_MODEL ** -0.5
    attn_width = N_HEADS * HEAD_DIM
    w_out = jax.random.normal(k_out, (attn_width, D_MODEL), jnp.float32) * (OUT_GAIN * attn_width ** -0.5)
    y_grad = jax.random.normal(k_dy, (BATCH_SIZE, SEQ_LEN, D_MODEL), jnp.float32)
    return {'x_seq': x_seq.astype(jnp.bfloat16), 'ln_gain': ln_gain.astype(jnp.bfloat16), 'w_qkv': w_qkv.reshape(D_MODEL, KV_HEADS, SLOT_WIDTH).astype(jnp.bfloat16), 'w_out': w_out.astype(jnp.bfloat16), 'y_grad': y_grad.astype(jnp.bfloat16)}


def rope_tables(seq_len):
    inv_freq = 1.0 / (ROPE_THETA ** (jnp.arange(0, HEAD_DIM, 2, dtype=jnp.float32) / HEAD_DIM))
    angles = jnp.arange(seq_len, dtype=jnp.float32)[:, None] * inv_freq[None, :]
    return jnp.cos(angles), jnp.sin(angles)


def rotate(vec_in, cos_t, sin_t):
    half_dim = vec_in.shape[-1] // 2
    half_lo = vec_in[..., :half_dim]
    half_hi = vec_in[..., half_dim:]
    return jnp.concatenate([half_lo * cos_t - half_hi * sin_t, half_hi * cos_t + half_lo * sin_t], axis=-1)


def group_attention(operands):
    query_rot, key_rot, val_head = operands
    scores = jnp.einsum('bqgd,bkd->bgqk', query_rot.astype(jnp.float32), key_rot.astype(jnp.float32)) * HEAD_DIM ** -0.5
    causal = jnp.arange(SEQ_LEN)[:, None] >= jnp.arange(SEQ_LEN)[None, :]
    scores = jnp.where(causal, scores, -1e30)
    attn_prob = jax.nn.softmax(scores, axis=-1).astype(jnp.bfloat16)
    return jnp.einsum('bgqk,bkd->bqgd', attn_prob.astype(jnp.float32), val_head.astype(jnp.float32)).astype(jnp.bfloat16)


def layer_forward(x_seq, ln_gain, w_qkv, w_out):
    x_f32 = x_seq.astype(jnp.float32)
    row_mean = jnp.mean(x_f32, axis=-1, keepdims=True)
    centered = x_f32 - row_mean
    variance = jnp.mean(centered * centered, axis=-1, keepdims=True)
    h_norm = (centered * lax.rsqrt(variance + LN_EPS) * ln_gain.astype(jnp.float32)).astype(jnp.bfloat16)
    qkv_raw = jnp.dot(h_norm.reshape(-1, D_MODEL).astype(jnp.float32), w_qkv.reshape(D_MODEL, -1).astype(jnp.float32)).astype(jnp.bfloat16)
    qkv_clip = jnp.where(jnp.abs(qkv_raw) < CLIP_QKV, qkv_raw, jnp.sign(qkv_raw) * CLIP_QKV)
    qkv_slots = qkv_clip.reshape(BATCH_SIZE, SEQ_LEN, KV_HEADS, GROUP_SIZE + 2, HEAD_DIM)
    cos_t, sin_t = rope_tables(SEQ_LEN)
    query_rot = rotate(qkv_slots[:, :, :, :GROUP_SIZE].astype(jnp.float32), cos_t[:, None, None], sin_t[:, None, None]).astype(jnp.bfloat16)
    key_rot = rotate(qkv_slots[:, :, :, GROUP_SIZE].astype(jnp.float32), cos_t[:, None], sin_t[:, None]).astype(jnp.bfloat16)
    val_head = qkv_slots[:, :, :, GROUP_SIZE + 1]
    mixed = lax.map(jax.checkpoint(group_attention), (jnp.moveaxis(query_rot, 2, 0), jnp.moveaxis(key_rot, 2, 0), jnp.moveaxis(val_head, 2, 0)))
    mixed = jnp.moveaxis(mixed, 0, 2).reshape(BATCH_SIZE * SEQ_LEN, N_HEADS * HEAD_DIM)
    out_proj = jnp.dot(mixed.astype(jnp.float32), w_out.astype(jnp.float32)).reshape(BATCH_SIZE, SEQ_LEN, D_MODEL)
    return (x_f32 + out_proj).astype(jnp.bfloat16)


def reference(x_seq, ln_gain, w_qkv, w_out, y_grad):
    y_out, pullback = jax.vjp(layer_forward, x_seq, ln_gain, w_qkv, w_out)
    x_grad, gain_grad, wqkv_grad, wout_grad = pullback(y_grad)
    return (y_out, x_grad, gain_grad, wqkv_grad, wout_grad)
```

```python
import functools
import jax
import jax.numpy as jnp
from jax import lax
from jax.experimental import pallas as pl
from jax.experimental.pallas import tpu as pltpu
from jax.sharding import PartitionSpec as P

CLIP_QKV = 8.0
ROPE_THETA = 500000.0
LN_EPS = 1e-5
LOG2E = 1.4426950408889634
HEAD_DIM = 128
TILE_Q = 256
NEG_BIG = -1e30
NT = (((1,), (1,)), ((), ()))
TN = (((0,), (0,)), ((), ()))
NN = (((1,), (0,)), ((), ()))


def dot(a, b, dims):
    return lax.dot_general(a, b, dims, preferred_element_type=jnp.float32)


def rope_tables(seq_len):
    inv_freq = 1.0 / (ROPE_THETA ** (jnp.arange(0, HEAD_DIM, 2, dtype=jnp.float32) / HEAD_DIM))
    angles = jnp.arange(seq_len, dtype=jnp.float32)[:, None] * inv_freq[None, :]
    cos_t, sin_t = jnp.cos(angles), jnp.sin(angles)
    return jnp.concatenate([cos_t, cos_t], axis=-1), jnp.concatenate([-sin_t, sin_t], axis=-1)


def clipped(raw):
    return jnp.minimum(jnp.maximum(raw.astype(jnp.float32), -CLIP_QKV), CLIP_QKV)


def rotate(vec, cos_t, sin_t):
    return (vec * cos_t + pltpu.roll(vec, HEAD_DIM // 2, 1) * sin_t).astype(jnp.bfloat16)


def unrotate(grad, cos_t, sin_t):
    grad = grad.astype(jnp.bfloat16).astype(jnp.float32)
    return grad * cos_t - pltpu.roll(grad, HEAD_DIM // 2, 1) * sin_t


def pass_clip(grad, raw):
    inside = jnp.abs(raw.astype(jnp.float32)) < CLIP_QKV
    return jnp.where(inside, grad, 0.0).astype(jnp.bfloat16)


def diagonal_mask():
    row = lax.broadcasted_iota(jnp.int32, (TILE_Q, TILE_Q), 0)
    col = lax.broadcasted_iota(jnp.int32, (TILE_Q, TILE_Q), 1)
    return row >= col


def mask_scores(scores, width, mask):
    tail = jnp.where(mask, scores[:, width - TILE_Q:], NEG_BIG)
    if width == TILE_Q:
        return tail
    return jnp.concatenate([scores[:, :width - TILE_Q], tail], axis=1)


def attn_fwd_kernel(groups, qkv_ref, cos_ref, sin_ref, out_ref, lse_ref, k_scr, v_scr):
    seq_len = qkv_ref.shape[0]
    k_col = groups * HEAD_DIM
    k_scr[...] = rotate(clipped(qkv_ref[:, k_col:k_col + HEAD_DIM]), cos_ref[...], sin_ref[...])
    v_scr[...] = clipped(qkv_ref[:, k_col + HEAD_DIM:k_col + 2 * HEAD_DIM]).astype(jnp.bfloat16)
    mask = diagonal_mask()
    coef = HEAD_DIM ** -0.5 * LOG2E

    def head(g, carry):
        cols = pl.ds(pl.multiple_of(g * HEAD_DIM, HEAD_DIM), HEAD_DIM)
        for qi in range(seq_len // TILE_Q):
            rows = slice(qi * TILE_Q, (qi + 1) * TILE_Q)
            width = (qi + 1) * TILE_Q
            query = rotate(clipped(qkv_ref[rows, cols]), cos_ref[rows, :], sin_ref[rows, :])
            scores = mask_scores(dot(query, k_scr[:width, :], NT), width, mask)
            peak = jnp.max(scores, axis=1, keepdims=True)
            prob = jnp.exp2((scores - peak) * coef)
            total = jnp.sum(prob, axis=1, keepdims=True)
            prob = (prob * (1.0 / total)).astype(jnp.bfloat16)
            out_ref[rows, cols] = dot(prob, v_scr[:width, :], NN).astype(jnp.bfloat16)
            lse = peak * coef + jnp.log2(total)
            lse_ref[rows, cols] = jnp.broadcast_to(lse, (TILE_Q, HEAD_DIM))
        return carry

    lax.fori_loop(0, groups, head, 0)


def attn_bwd_kernel(groups, qkv_ref, attn_ref, dattn_ref, lse_ref, cos_ref, sin_ref, dqkv_ref, k_scr, v_scr, dk_scr, dv_scr):
    seq_len = qkv_ref.shape[0]
    k_col = groups * HEAD_DIM
    v_col = k_col + HEAD_DIM
    scale = HEAD_DIM ** -0.5
    coef = scale * LOG2E
    k_scr[...] = rotate(clipped(qkv_ref[:, k_col:v_col]), cos_ref[...], sin_ref[...])
    v_scr[...] = clipped(qkv_ref[:, v_col:v_col + HEAD_DIM]).astype(jnp.bfloat16)
    dk_scr[...] = jnp.zeros_like(dk_scr)
    dv_scr[...] = jnp.zeros_like(dv_scr)
    mask = diagonal_mask()

    def head(g, carry):
        cols = pl.ds(pl.multiple_of(g * HEAD_DIM, HEAD_DIM), HEAD_DIM)
        for qi in range(seq_len // TILE_Q):
            rows = slice(qi * TILE_Q, (qi + 1) * TILE_Q)
            width = (qi + 1) * TILE_Q
            raw = qkv_ref[rows, cols]
            cos_t, sin_t = cos_ref[rows, :], sin_ref[rows, :]
            query = rotate(clipped(raw), cos_t, sin_t)
            dout = dattn_ref[rows, cols]
            delta = jnp.sum(dout.astype(jnp.float32) * attn_ref[rows, cols].astype(jnp.float32), axis=1, keepdims=True)
            scores = mask_scores(dot(query, k_scr[:width, :], NT), width, mask)
            lse = jnp.concatenate([lse_ref[rows, cols]] * (width // HEAD_DIM), axis=1)
            prob = jnp.exp2(scores * coef - lse)
            dprob = dot(dout, v_scr[:width, :], NT).astype(jnp.bfloat16).astype(jnp.float32)
            dscore = (prob * (dprob - delta)).astype(jnp.bfloat16)
            prob = prob.astype(jnp.bfloat16)
            dv_scr[:, :width] += dot(dout, prob, TN)
            dk_scr[:, :width] += dot(query, dscore, TN)
            dquery = dot(dscore, k_scr[:width, :], NN) * scale
            dqkv_ref[rows, cols] = pass_clip(unrotate(dquery, cos_t, sin_t), raw)
        return carry

    lax.fori_loop(0, groups, head, 0)
    dkey = unrotate(dk_scr[...].T * scale, cos_ref[...], sin_ref[...])
    dqkv_ref[:, k_col:v_col] = pass_clip(dkey, qkv_ref[:, k_col:v_col])
    dqkv_ref[:, v_col:v_col + HEAD_DIM] = pass_clip(dv_scr[...].T, qkv_ref[:, v_col:v_col + HEAD_DIM])


def attn_fwd(qkv, cos_t, sin_t, kv_loc):
    seq_len = qkv.shape[0]
    slot = qkv.shape[1] // kv_loc
    groups = slot // HEAD_DIM - 2
    wide = groups * HEAD_DIM
    table = pl.BlockSpec((seq_len, HEAD_DIM), lambda n: (0, 0))
    return pl.pallas_call(
        functools.partial(attn_fwd_kernel, groups),
        grid=(kv_loc,),
        in_specs=[pl.BlockSpec((seq_len, slot), lambda n: (0, n)), table, table],
        out_specs=[pl.BlockSpec((seq_len, wide), lambda n: (0, n))] * 2,
        out_shape=[jax.ShapeDtypeStruct((seq_len, kv_loc * wide), jnp.bfloat16), jax.ShapeDtypeStruct((seq_len, kv_loc * wide), jnp.float32)],
        scratch_shapes=[pltpu.VMEM((seq_len, HEAD_DIM), jnp.bfloat16)] * 2,
        compiler_params=pltpu.CompilerParams(vmem_limit_bytes=48 * 2 ** 20),
        cost_estimate=pl.CostEstimate(flops=12 * 10 ** 9, bytes_accessed=14 * 10 ** 6, transcendentals=0),
        name="attn_fwd",
    )(qkv, cos_t, sin_t)


def attn_bwd(qkv, attn, dattn, lse, cos_t, sin_t, kv_loc):
    seq_len = qkv.shape[0]
    slot = qkv.shape[1] // kv_loc
    groups = slot // HEAD_DIM - 2
    wide = groups * HEAD_DIM
    table = pl.BlockSpec((seq_len, HEAD_DIM), lambda n: (0, 0))
    part = pl.BlockSpec((seq_len, wide), lambda n: (0, n))
    full = pl.BlockSpec((seq_len, slot), lambda n: (0, n))
    return pl.pallas_call(
        functools.partial(attn_bwd_kernel, groups),
        grid=(kv_loc,),
        in_specs=[full, part, part, part, table, table],
        out_specs=full,
        out_shape=jax.ShapeDtypeStruct(qkv.shape, jnp.bfloat16),
        scratch_shapes=[pltpu.VMEM((seq_len, HEAD_DIM), jnp.bfloat16)] * 2 + [pltpu.VMEM((HEAD_DIM, seq_len), jnp.float32)] * 2,
        compiler_params=pltpu.CompilerParams(vmem_limit_bytes=56 * 2 ** 20),
        cost_estimate=pl.CostEstimate(flops=25 * 10 ** 9, bytes_accessed=22 * 10 ** 6, transcendentals=0),
        name="attn_bwd",
    )(qkv, attn, dattn, lse, cos_t, sin_t)


def dw_qkv_kernel(h0_ref, h1_ref, g0_ref, g1_ref, out_ref):
    slot = out_ref.shape[2]
    for n in range(out_ref.shape[1]):
        cols = slice(n * slot, (n + 1) * slot)
        acc = dot(h0_ref[...], g0_ref[:, cols], TN) + dot(h1_ref[...], g1_ref[:, cols], TN)
        out_ref[:, n, :] = acc.astype(jnp.bfloat16)


def dw_qkv(h0, h1, g0, g1, kv_loc, tile=512):
    seq_len, d_model = h0.shape
    width = g0.shape[1]
    slot = width // kv_loc
    whole = pl.BlockSpec((seq_len, width), lambda i: (0, 0))
    part = pl.BlockSpec((seq_len, tile), lambda i: (0, i))
    return pl.pallas_call(
        dw_qkv_kernel,
        grid=(d_model // tile,),
        in_specs=[part, part, whole, whole],
        out_specs=pl.BlockSpec((tile, kv_loc, slot), lambda i: (i, 0, 0)),
        out_shape=jax.ShapeDtypeStruct((d_model, kv_loc, slot), jnp.bfloat16),
        compiler_params=pltpu.CompilerParams(vmem_limit_bytes=60 * 2 ** 20),
        cost_estimate=pl.CostEstimate(flops=51 * 10 ** 9, bytes_accessed=60 * 10 ** 6, transcendentals=0),
        name="dw_qkv",
    )(h0, h1, g0, g1)


def dw_out_kernel(a0_ref, a1_ref, g0_ref, g1_ref, out_ref):
    acc = dot(a0_ref[...], g0_ref[...], TN) + dot(a1_ref[...], g1_ref[...], TN)
    out_ref[...] = acc.astype(jnp.bfloat16)


def dw_out(a0, a1, g0, g1, tile=512):
    seq_len, width = a0.shape
    d_model = g0.shape[1]
    whole = pl.BlockSpec((seq_len, width), lambda i: (0, 0))
    part = pl.BlockSpec((seq_len, tile), lambda i: (0, i))
    return pl.pallas_call(
        dw_out_kernel,
        grid=(d_model // tile,),
        in_specs=[whole, whole, part, part],
        out_specs=pl.BlockSpec((width, tile), lambda i: (0, i)),
        out_shape=jax.ShapeDtypeStruct((width, d_model), jnp.bfloat16),
        compiler_params=pltpu.CompilerParams(vmem_limit_bytes=60 * 2 ** 20),
        cost_estimate=pl.CostEstimate(flops=39 * 10 ** 9, bytes_accessed=50 * 10 ** 6, transcendentals=0),
        name="dw_out",
    )(a0, a1, g0, g1)


def norm_stats(x_f32):
    centered = x_f32 - jnp.mean(x_f32, axis=-1, keepdims=True)
    return centered * lax.rsqrt(jnp.mean(centered * centered, axis=-1, keepdims=True) + LN_EPS)


def norm_stat_pair(x_f32):
    mean = jnp.mean(x_f32, axis=-1, keepdims=True)
    centered = x_f32 - mean
    return mean, lax.rsqrt(jnp.mean(centered * centered, axis=-1, keepdims=True) + LN_EPS)


def solution(mesh):
    n_tp = mesh.shape["tp"]

    def swap(value, bit):
        return lax.ppermute(value, "tp", [(i, i ^ bit) for i in range(n_tp)])

    def device_step(x_seq, ln_gain, w_qkv, w_out, y_grad):
        batch, kv_loc = x_seq.shape[0], w_qkv.shape[1]
        gain = ln_gain.astype(jnp.float32)
        w_flat = w_qkv.reshape(w_qkv.shape[0], -1)
        xs = [x_seq[b].astype(jnp.float32) for b in range(batch)]
        dys = [y_grad[b] for b in range(batch)]
        stats = [norm_stat_pair(x) for x in xs]
        hats = [(x - m) * r for x, (m, r) in zip(xs, stats)]
        cos_t, sin_t = rope_tables(x_seq.shape[1] * n_tp)
        hs = [lax.all_gather((hat * gain).astype(jnp.bfloat16), "tp", axis=0, tiled=True) for hat in hats]
        dy_full = [lax.all_gather(dy, "tp", axis=0, tiled=True) for dy in dys]
        qkvs, attns, lses, outs = [], [], [], []
        for b in range(batch):
            qkv = dot(hs[b], w_flat, NN).astype(jnp.bfloat16)
            attn, lse = attn_fwd(qkv, cos_t, sin_t, kv_loc)
            out_part = dot(attn, w_out, NN).astype(jnp.bfloat16)
            outs.append(lax.psum_scatter(out_part, "tp", scatter_dimension=0, tiled=True))
            qkvs.append(qkv)
            attns.append(attn)
            lses.append(lse)
        dqkvs, dhs = [], []
        for b in range(batch):
            dattn = dot(dy_full[b], w_out, NT).astype(jnp.bfloat16)
            dqkv = attn_bwd(qkvs[b], attns[b], dattn, lses[b], cos_t, sin_t, kv_loc)
            dh_part = dot(dqkv, w_flat, NT).astype(jnp.bfloat16)
            dhs.append(lax.psum_scatter(dh_part, "tp", scatter_dimension=0, tiled=True))
            dqkvs.append(dqkv)
        wout_grad = dw_out(attns[0], attns[1], dy_full[0], dy_full[1])
        wqkv_grad = dw_qkv(hs[0], hs[1], dqkvs[0], dqkvs[1], kv_loc)
        y_out = jnp.stack([(x + o.astype(jnp.float32)).astype(jnp.bfloat16) for x, o in zip(xs, outs)])
        gain_part, dxs = 0.0, []
        for b in range(batch):
            dh = dhs[b].astype(jnp.float32)
            gain_part = gain_part + jnp.sum(dh * hats[b], axis=0)
            dhat = dh * gain
            inner = dhat - jnp.mean(dhat, axis=-1, keepdims=True) - hats[b] * jnp.mean(dhat * hats[b], axis=-1, keepdims=True)
            dxs.append((dys[b].astype(jnp.float32) + inner * stats[b][1]).astype(jnp.bfloat16))
        gain_part = gain_part + swap(gain_part, 1)
        gain_grad = (gain_part + swap(gain_part, 2)).astype(jnp.bfloat16)
        return y_out, jnp.stack(dxs), gain_grad, wqkv_grad, wout_grad

    specs_in = (P('dp', 'tp', None), P(None), P(None, 'tp', None), P('tp', None), P('dp', 'tp', None))
    specs_out = (P('dp', 'tp', None), P('dp', 'tp', None), P('dp'), P('dp', 'tp', None), P(('dp', 'tp'), None))
    return jax.shard_map(device_step, mesh=mesh, in_specs=specs_in, out_specs=specs_out, check_vma=False)
```

```python
import functools
import jax
import jax.numpy as jnp
from jax import lax
from jax.experimental import pallas as pl
from jax.experimental.pallas import tpu as pltpu
from jax.sharding import PartitionSpec as P

CLIP_QKV = 8.0
ROPE_THETA = 500000.0
LN_EPS = 1e-5
LOG2E = 1.4426950408889634
HEAD_DIM = 128
TILE_Q = 256
NEG_BIG = -1e30
NT = (((1,), (1,)), ((), ()))
TN = (((0,), (0,)), ((), ()))
NN = (((1,), (0,)), ((), ()))


def dot(a, b, dims):
    return lax.dot_general(a, b, dims, preferred_element_type=jnp.float32)


def rope_tables(seq_len):
    inv_freq = 1.0 / (ROPE_THETA ** (jnp.arange(0, HEAD_DIM, 2, dtype=jnp.float32) / HEAD_DIM))
    angles = jnp.arange(seq_len, dtype=jnp.float32)[:, None] * inv_freq[None, :]
    cos_t, sin_t = jnp.cos(angles), jnp.sin(angles)
    return jnp.concatenate([cos_t, cos_t], axis=-1), jnp.concatenate([-sin_t, sin_t], axis=-1)


def clipped(raw):
    return jnp.minimum(jnp.maximum(raw.astype(jnp.float32), -CLIP_QKV), CLIP_QKV)


def rotate(vec, cos_t, sin_t):
    return (vec * cos_t + pltpu.roll(vec, HEAD_DIM // 2, 1) * sin_t).astype(jnp.bfloat16)


def unrotate(grad, cos_t, sin_t):
    grad = grad.astype(jnp.bfloat16).astype(jnp.float32)
    return grad * cos_t - pltpu.roll(grad, HEAD_DIM // 2, 1) * sin_t


def pass_clip(grad, raw):
    inside = jnp.abs(raw.astype(jnp.float32)) < CLIP_QKV
    return jnp.where(inside, grad, 0.0).astype(jnp.bfloat16)


def diagonal_mask():
    row = lax.broadcasted_iota(jnp.int32, (TILE_Q, TILE_Q), 0)
    col = lax.broadcasted_iota(jnp.int32, (TILE_Q, TILE_Q), 1)
    return row >= col


def mask_scores(scores, width, mask):
    tail = jnp.where(mask, scores[:, width - TILE_Q:], NEG_BIG)
    if width == TILE_Q:
        return tail
    return jnp.concatenate([scores[:, :width - TILE_Q], tail], axis=1)


def half_rows(own, size):
    side = lax.axis_index("tp") // 2
    start = side if own else 1 - side
    return pl.ds(pl.multiple_of(start * size, size), size)


def attn_fwd_kernel(groups, own_ref, far_ref, cos_ref, sin_ref, oown_ref, ofar_ref, lse_ref, qkv_ref, out_ref, k_scr, v_scr):
    half = own_ref.shape[0]
    own, far = half_rows(True, half), half_rows(False, half)
    qkv_ref[own, :] = own_ref[...]
    qkv_ref[far, :] = far_ref[...]
    seq_len = qkv_ref.shape[0]
    k_col = groups * HEAD_DIM
    k_scr[...] = rotate(clipped(qkv_ref[:, k_col:k_col + HEAD_DIM]), cos_ref[...], sin_ref[...])
    v_scr[...] = clipped(qkv_ref[:, k_col + HEAD_DIM:k_col + 2 * HEAD_DIM]).astype(jnp.bfloat16)
    mask = diagonal_mask()
    coef = HEAD_DIM ** -0.5 * LOG2E

    def head(g, carry):
        cols = pl.ds(pl.multiple_of(g * HEAD_DIM, HEAD_DIM), HEAD_DIM)
        for qi in range(seq_len // TILE_Q):
            rows = slice(qi * TILE_Q, (qi + 1) * TILE_Q)
            width = (qi + 1) * TILE_Q
            query = rotate(clipped(qkv_ref[rows, cols]), cos_ref[rows, :], sin_ref[rows, :])
            scores = mask_scores(dot(query, k_scr[:width, :], NT), width, mask)
            peak = jnp.max(scores, axis=1, keepdims=True)
            prob = jnp.exp2((scores - peak) * coef)
            total = jnp.sum(prob, axis=1, keepdims=True)
            prob = (prob * (1.0 / total)).astype(jnp.bfloat16)
            out_ref[rows, cols] = dot(prob, v_scr[:width, :], NN).astype(jnp.bfloat16)
            lse = peak * coef + jnp.log2(total)
            lse_ref[rows, cols] = jnp.broadcast_to(lse, (TILE_Q, HEAD_DIM))
        return carry

    lax.fori_loop(0, groups, head, 0)
    oown_ref[...] = out_ref[own, :]
    ofar_ref[...] = out_ref[far, :]


def attn_bwd_kernel(groups, own_ref, far_ref, aown_ref, afar_ref, down_ref, dfar_ref, lse_ref, cos_ref, sin_ref, gown_ref, gfar_ref, qkv_ref, attn_ref, dattn_ref, k_scr, v_scr, dk_scr, dv_scr):
    half = own_ref.shape[0]
    own, far = half_rows(True, half), half_rows(False, half)
    for dst, near, away in ((qkv_ref, own_ref, far_ref), (attn_ref, aown_ref, afar_ref), (dattn_ref, down_ref, dfar_ref)):
        dst[own, :] = near[...]
        dst[far, :] = away[...]
    seq_len = qkv_ref.shape[0]
    k_col = groups * HEAD_DIM
    v_col = k_col + HEAD_DIM
    scale = HEAD_DIM ** -0.5
    coef = scale * LOG2E
    k_scr[...] = rotate(clipped(qkv_ref[:, k_col:v_col]), cos_ref[...], sin_ref[...])
    v_scr[...] = clipped(qkv_ref[:, v_col:v_col + HEAD_DIM]).astype(jnp.bfloat16)
    dk_scr[...] = jnp.zeros_like(dk_scr)
    dv_scr[...] = jnp.zeros_like(dv_scr)
    mask = diagonal_mask()

    def head(g, carry):
        cols = pl.ds(pl.multiple_of(g * HEAD_DIM, HEAD_DIM), HEAD_DIM)
        for qi in range(seq_len // TILE_Q):
            rows = slice(qi * TILE_Q, (qi + 1) * TILE_Q)
            width = (qi + 1) * TILE_Q
            raw = qkv_ref[rows, cols]
            cos_t, sin_t = cos_ref[rows, :], sin_ref[rows, :]
            query = rotate(clipped(raw), cos_t, sin_t)
            dout = dattn_ref[rows, cols]
            delta = jnp.sum(dout.astype(jnp.float32) * attn_ref[rows, cols].astype(jnp.float32), axis=1, keepdims=True)
            scores = mask_scores(dot(query, k_scr[:width, :], NT), width, mask)
            lse = jnp.concatenate([lse_ref[rows, cols]] * (width // HEAD_DIM), axis=1)
            prob = jnp.exp2(scores * coef - lse)
            dprob = dot(dout, v_scr[:width, :], NT).astype(jnp.bfloat16).astype(jnp.float32)
            dscore = (prob * (dprob - delta)).astype(jnp.bfloat16)
            prob = prob.astype(jnp.bfloat16)
            dv_scr[:, :width] += dot(dout, prob, TN)
            dk_scr[:, :width] += dot(query, dscore, TN)
            dquery = dot(dscore, k_scr[:width, :], NN) * scale
            qkv_ref[rows, cols] = pass_clip(unrotate(dquery, cos_t, sin_t), raw)
        return carry

    lax.fori_loop(0, groups, head, 0)
    dkey = unrotate(dk_scr[...].T * scale, cos_ref[...], sin_ref[...])
    qkv_ref[:, k_col:v_col] = pass_clip(dkey, qkv_ref[:, k_col:v_col])
    qkv_ref[:, v_col:v_col + HEAD_DIM] = pass_clip(dv_scr[...].T, qkv_ref[:, v_col:v_col + HEAD_DIM])
    gown_ref[...] = qkv_ref[own, :]
    gfar_ref[...] = qkv_ref[far, :]


def head_specs(half, slot, wide):
    table = pl.BlockSpec((2 * half, HEAD_DIM), lambda n: (0, 0))
    part = pl.BlockSpec((half, wide), lambda n: (0, n))
    full = pl.BlockSpec((half, slot), lambda n: (0, n))
    lse = pl.BlockSpec((2 * half, wide), lambda n: (0, n))
    return table, part, full, lse


def attn_fwd(qkv_own, qkv_far, cos_t, sin_t, kv_loc):
    half = qkv_own.shape[0]
    slot = qkv_own.shape[1] // kv_loc
    groups = slot // HEAD_DIM - 2
    wide = groups * HEAD_DIM
    table, part, full, lse = head_specs(half, slot, wide)
    rows = jax.ShapeDtypeStruct((half, kv_loc * wide), jnp.bfloat16)
    return pl.pallas_call(
        functools.partial(attn_fwd_kernel, groups),
        grid=(kv_loc,),
        in_specs=[full, full, table, table],
        out_specs=[part, part, lse],
        out_shape=[rows, rows, jax.ShapeDtypeStruct((2 * half, kv_loc * wide), jnp.float32)],
        scratch_shapes=[pltpu.VMEM((2 * half, slot), jnp.bfloat16), pltpu.VMEM((2 * half, wide), jnp.bfloat16)] + [pltpu.VMEM((2 * half, HEAD_DIM), jnp.bfloat16)] * 2,
        compiler_params=pltpu.CompilerParams(vmem_limit_bytes=48 * 2 ** 20),
        cost_estimate=pl.CostEstimate(flops=12 * 10 ** 9, bytes_accessed=14 * 10 ** 6, transcendentals=0),
        name="attn_fwd",
    )(qkv_own, qkv_far, cos_t, sin_t)


def attn_bwd(qkv_own, qkv_far, attn_own, attn_far, dattn_own, dattn_far, lse_t, cos_t, sin_t, kv_loc):
    half = qkv_own.shape[0]
    slot = qkv_own.shape[1] // kv_loc
    groups = slot // HEAD_DIM - 2
    wide = groups * HEAD_DIM
    table, part, full, lse = head_specs(half, slot, wide)
    return pl.pallas_call(
        functools.partial(attn_bwd_kernel, groups),
        grid=(kv_loc,),
        in_specs=[full, full, part, part, part, part, lse, table, table],
        out_specs=[full, full],
        out_shape=[jax.ShapeDtypeStruct(qkv_own.shape, jnp.bfloat16)] * 2,
        scratch_shapes=[pltpu.VMEM((2 * half, slot), jnp.bfloat16)] + [pltpu.VMEM((2 * half, wide), jnp.bfloat16)] * 2 + [pltpu.VMEM((2 * half, HEAD_DIM), jnp.bfloat16)] * 2 + [pltpu.VMEM((HEAD_DIM, 2 * half), jnp.float32)] * 2,
        compiler_params=pltpu.CompilerParams(vmem_limit_bytes=56 * 2 ** 20),
        cost_estimate=pl.CostEstimate(flops=25 * 10 ** 9, bytes_accessed=22 * 10 ** 6, transcendentals=0),
        name="attn_bwd",
    )(qkv_own, qkv_far, attn_own, attn_far, dattn_own, dattn_far, lse_t, cos_t, sin_t)


def dw_qkv_kernel(n_rows, *refs):
    acts, grads, out_ref = refs[:n_rows], refs[n_rows:-1], refs[-1]
    slot = out_ref.shape[2]
    for n in range(out_ref.shape[1]):
        cols = slice(n * slot, (n + 1) * slot)
        acc = sum(dot(a[...], g[:, cols], TN) for a, g in zip(acts, grads))
        out_ref[:, n, :] = acc.astype(jnp.bfloat16)


def dw_qkv(acts, grads, kv_loc, tile=512):
    rows, d_model = acts[0].shape
    width = grads[0].shape[1]
    slot = width // kv_loc
    whole = pl.BlockSpec((rows, width), lambda i: (0, 0))
    part = pl.BlockSpec((rows, tile), lambda i: (0, i))
    return pl.pallas_call(
        functools.partial(dw_qkv_kernel, len(acts)),
        grid=(d_model // tile,),
        in_specs=[part] * len(acts) + [whole] * len(grads),
        out_specs=pl.BlockSpec((tile, kv_loc, slot), lambda i: (i, 0, 0)),
        out_shape=jax.ShapeDtypeStruct((d_model, kv_loc, slot), jnp.bfloat16),
        compiler_params=pltpu.CompilerParams(vmem_limit_bytes=60 * 2 ** 20),
        cost_estimate=pl.CostEstimate(flops=51 * 10 ** 9, bytes_accessed=60 * 10 ** 6, transcendentals=0),
        name="dw_qkv",
    )(*acts, *grads)


def dw_out_kernel(n_rows, *refs):
    acts, grads, out_ref = refs[:n_rows], refs[n_rows:-1], refs[-1]
    out_ref[...] = sum(dot(a[...], g[...], TN) for a, g in zip(acts, grads)).astype(jnp.bfloat16)


def dw_out(acts, grads, tile=512):
    rows, width = acts[0].shape
    d_model = grads[0].shape[-1]
    whole = pl.BlockSpec((rows, width), lambda i: (0, 0))
    part = pl.BlockSpec((rows, tile), lambda i: (0, i))
    return pl.pallas_call(
        functools.partial(dw_out_kernel, len(acts)),
        grid=(d_model // tile,),
        in_specs=[whole] * len(acts) + [part] * len(grads),
        out_specs=pl.BlockSpec((width, tile), lambda i: (0, i)),
        out_shape=jax.ShapeDtypeStruct((width, d_model), jnp.bfloat16),
        compiler_params=pltpu.CompilerParams(vmem_limit_bytes=60 * 2 ** 20),
        cost_estimate=pl.CostEstimate(flops=39 * 10 ** 9, bytes_accessed=50 * 10 ** 6, transcendentals=0),
        name="dw_out",
    )(*acts, *grads)


def normalized(x_f32):
    centered = x_f32 - jnp.mean(x_f32, axis=-1, keepdims=True)
    rstd = lax.rsqrt(jnp.mean(centered * centered, axis=-1, keepdims=True) + LN_EPS)
    return centered * rstd, rstd


def norm_fwd_kernel(x_ref, gain_ref, h_ref):
    hat, _ = normalized(x_ref[0].astype(jnp.float32))
    h_ref[...] = (hat * gain_ref[...]).astype(jnp.bfloat16)


def norm_fwd(x_seq, gain, b, tile=64):
    _, rows, d_model = x_seq.shape
    return pl.pallas_call(
        norm_fwd_kernel,
        grid=(rows // tile,),
        in_specs=[pl.BlockSpec((1, tile, d_model), lambda i: (b, i, 0)), pl.BlockSpec((1, d_model), lambda i: (0, 0))],
        out_specs=pl.BlockSpec((tile, d_model), lambda i: (i, 0)),
        out_shape=jax.ShapeDtypeStruct((rows, d_model), jnp.bfloat16),
        cost_estimate=pl.CostEstimate(flops=2 * 10 ** 9, bytes_accessed=7 * 10 ** 6, transcendentals=0),
        name="norm_fwd",
    )(x_seq, gain)


def residual_kernel(x_ref, near_ref, far_ref, *rest):
    total = near_ref[...].astype(jnp.float32) + far_ref[...].astype(jnp.float32)
    rest[-1][0] = (x_ref[0].astype(jnp.float32) + total.astype(jnp.bfloat16).astype(jnp.float32)).astype(jnp.bfloat16)


def norm_bwd_kernel(x_ref, dy_ref, gain_ref, near_ref, far_ref, *rest):
    dx_ref, dgain_ref = rest[-2:]
    hat, rstd = normalized(x_ref[0].astype(jnp.float32))
    dh = (near_ref[...].astype(jnp.float32) + far_ref[...].astype(jnp.float32)).astype(jnp.bfloat16).astype(jnp.float32)

    @pl.when(pl.program_id(0) == 0)
    def _():
        dgain_ref[...] = jnp.zeros_like(dgain_ref)

    dgain_ref[...] += jnp.sum(dh * hat, axis=0, keepdims=True)
    dhat = dh * gain_ref[...]
    inner = dhat - jnp.mean(dhat, axis=-1, keepdims=True) - hat * jnp.mean(dhat * hat, axis=-1, keepdims=True)
    dx_ref[0] = (dy_ref[0].astype(jnp.float32) + inner * rstd).astype(jnp.bfloat16)


def residual(x_seq, near, far, b, held, tile=64):
    _, rows, d_model = x_seq.shape
    whole = pl.BlockSpec((1, tile, d_model), lambda i: (b, i, 0))
    part = pl.BlockSpec((tile, d_model), lambda i: (i, 0))
    keep = [] if held is None else [held]
    return pl.pallas_call(
        residual_kernel,
        grid=(rows // tile,),
        in_specs=[whole, part, part] + [pl.BlockSpec(memory_space=pl.ANY)] * len(keep),
        out_specs=whole,
        out_shape=jax.ShapeDtypeStruct(x_seq.shape, jnp.bfloat16),
        input_output_aliases={3: 0} if keep else {},
        cost_estimate=pl.CostEstimate(flops=2 * 10 ** 9, bytes_accessed=13 * 10 ** 6, transcendentals=0),
        name="residual",
    )(x_seq, near, far, *keep)


def norm_bwd(x_seq, y_grad, gain, near, far, b, held, tile=64):
    _, rows, d_model = x_seq.shape
    whole = pl.BlockSpec((1, tile, d_model), lambda i: (b, i, 0))
    part = pl.BlockSpec((tile, d_model), lambda i: (i, 0))
    row = pl.BlockSpec((1, d_model), lambda i: (0, 0))
    keep = [] if held is None else [held]
    return pl.pallas_call(
        norm_bwd_kernel,
        grid=(rows // tile,),
        in_specs=[whole, whole, row, part, part] + [pl.BlockSpec(memory_space=pl.ANY)] * len(keep),
        out_specs=[whole, row],
        out_shape=[jax.ShapeDtypeStruct(x_seq.shape, jnp.bfloat16), jax.ShapeDtypeStruct((1, d_model), jnp.float32)],
        input_output_aliases={5: 0} if keep else {},
        cost_estimate=pl.CostEstimate(flops=4 * 10 ** 9, bytes_accessed=16 * 10 ** 6, transcendentals=0),
        name="norm_bwd",
    )(x_seq, y_grad, gain, near, far, *keep)


def solution(mesh):
    n_tp = mesh.shape["tp"]
    pairs = [[i, i + 1] for i in range(0, n_tp, 2)]

    def swap(value, bit):
        return lax.ppermute(value, "tp", [(i, i ^ bit) for i in range(n_tp)])

    def pair_gather(value):
        return lax.all_gather(value, "tp", axis_index_groups=pairs, axis=0, tiled=True)

    def pair_scatter(value):
        return lax.psum_scatter(value, "tp", axis_index_groups=pairs, scatter_dimension=0, tiled=True)

    def staged_step(x_seq, ln_gain, w_qkv, w_out, y_grad):
        kv_loc = w_qkv.shape[1]
        gain = ln_gain.astype(jnp.float32)[None, :]
        token = [None]

        def run(fn, lead, *rest):
            if token[0] is not None:
                lead, _ = lax.optimization_barrier((lead, token[0]))
            result = fn(lead, *rest)
            token[0] = jax.tree.leaves(result)[0]
            return result

        def matmul(dims):
            return lambda a, b: dot(a, b, dims).astype(jnp.bfloat16)

        cos_t, sin_t = rope_tables(x_seq.shape[1] * n_tp)
        h0 = run(lambda x: norm_fwd(x, gain, 0), x_seq)
        hx0 = swap(h0, 2)
        h1 = run(lambda x: norm_fwd(x, gain, 1), x_seq)
        hx1 = swap(h1, 2)
        dy0, dy1, _ = lax.optimization_barrier((y_grad[0], y_grad[1], h1))
        dyx0 = swap(dy0, 2)
        dyx1 = swap(dy1, 2)
        h_own0, h_own1 = pair_gather(h0), pair_gather(h1)
        dy_own0, dy_own1 = pair_gather(dy0), pair_gather(dy1)
        w_flat = run(lambda w: lax.optimization_barrier(w.reshape(w.shape[0], -1)), w_qkv)
        qkv_own0 = run(matmul(NN), h_own0, w_flat)
        qkv_own1 = run(matmul(NN), h_own1, w_flat)
        h_far0 = pair_gather(hx0)
        dattn_own0 = run(matmul(NT), dy_own0, w_out)
        qkv_far0 = run(matmul(NN), h_far0, w_flat)
        attn_own0, attn_far0, lse0 = run(lambda far: attn_fwd(qkv_own0, far, cos_t, sin_t, kv_loc), qkv_far0)
        o_far0 = run(matmul(NN), attn_far0, w_out)
        h_far1 = pair_gather(hx1)
        os_far0 = pair_scatter(o_far0)
        o_near0 = run(matmul(NN), attn_own0, w_out)
        ox0 = swap(os_far0, 2)
        os_near0 = pair_scatter(o_near0)
        dattn_own1 = run(matmul(NT), dy_own1, w_out)
        qkv_far1 = run(matmul(NN), h_far1, w_flat)
        attn_own1, attn_far1, lse1 = run(lambda far: attn_fwd(qkv_own1, far, cos_t, sin_t, kv_loc), qkv_far1)
        dy_far0 = pair_gather(dyx0)
        o_far1 = run(matmul(NN), attn_far1, w_out)
        os_far1 = pair_scatter(o_far1)
        dattn_far0 = run(matmul(NT), dy_far0, w_out)
        ox1 = swap(os_far1, 2)
        dq_own0, dq_far0 = run(lambda d: attn_bwd(qkv_own0, qkv_far0, attn_own0, attn_far0, dattn_own0, d, lse0, cos_t, sin_t, kv_loc), dattn_far0)
        dy_far1 = pair_gather(dyx1)
        dh_far0 = run(matmul(NT), dq_far0, w_flat)
        dhs_far0 = pair_scatter(dh_far0)
        o_near1 = run(matmul(NN), attn_own1, w_out)
        dhx0 = swap(dhs_far0, 2)
        os_near1 = pair_scatter(o_near1)
        dattn_far1 = run(matmul(NT), dy_far1, w_out)
        dq_own1, dq_far1 = run(lambda d: attn_bwd(qkv_own1, qkv_far1, attn_own1, attn_far1, dattn_own1, d, lse1, cos_t, sin_t, kv_loc), dattn_far1)
        dh_far1 = run(matmul(NT), dq_far1, w_flat)
        dhs_far1 = pair_scatter(dh_far1)
        dh_near0 = run(matmul(NT), dq_own0, w_flat)
        dhx1 = swap(dhs_far1, 2)
        dhs_near0 = pair_scatter(dh_near0)
        dh_near1 = run(matmul(NT), dq_own1, w_flat)
        dhs_near1 = pair_scatter(dh_near1)
        wout_grad = run(lambda a: dw_out([a, attn_far0, attn_own1, attn_far1], [dy_own0, dy_far0, dy_own1, dy_far1]), attn_own0)
        y_out = run(lambda near: residual(x_seq, near, ox0, 0, None), os_near0)
        y_out = run(lambda near: residual(x_seq, near, ox1, 1, y_out), os_near1)
        wqkv_grad = run(lambda h: dw_qkv([h, h_far0, h_own1, h_far1], [dq_own0, dq_far0, dq_own1, dq_far1], kv_loc), h_own0)
        x_grad, gain0 = run(lambda near: norm_bwd(x_seq, y_grad, gain, near, dhx0, 0, None), dhs_near0)
        x_grad, gain1 = run(lambda near: norm_bwd(x_seq, y_grad, gain, near, dhx1, 1, x_grad), dhs_near1)
        gain_part = gain0 + gain1
        gain_part = gain_part + swap(gain_part, 1)
        gain_grad = (gain_part + swap(gain_part, 2)).astype(jnp.bfloat16)[0]
        return y_out, x_grad, gain_grad, wqkv_grad, wout_grad

    specs_in = (P('dp', 'tp', None), P(None), P(None, 'tp', None), P('tp', None), P('dp', 'tp', None))
    specs_out = (P('dp', 'tp', None), P('dp', 'tp', None), P('dp'), P('dp', 'tp', None), P(('dp', 'tp'), None))
    return jax.shard_map(staged_step, mesh=mesh, in_specs=specs_in, out_specs=specs_out, check_vma=False)
```

```python
import functools
import jax
import jax.numpy as jnp
from jax import lax
from jax.experimental import pallas as pl
from jax.experimental.pallas import tpu as pltpu
from jax.sharding import PartitionSpec as P

CLIP_QKV = 8.0
ROPE_THETA = 500000.0
LN_EPS = 1e-5
LOG2E = 1.4426950408889634
HEAD_DIM = 128
TILE_Q = 256
NEG_BIG = -1e30
NT = (((1,), (1,)), ((), ()))
TN = (((0,), (0,)), ((), ()))
NN = (((1,), (0,)), ((), ()))


def dot(a, b, dims):
    return lax.dot_general(a, b, dims, preferred_element_type=jnp.float32)


def rope_tables(seq_len):
    inv_freq = 1.0 / (ROPE_THETA ** (jnp.arange(0, HEAD_DIM, 2, dtype=jnp.float32) / HEAD_DIM))
    angles = jnp.arange(seq_len, dtype=jnp.float32)[:, None] * inv_freq[None, :]
    cos_t, sin_t = jnp.cos(angles), jnp.sin(angles)
    return jnp.concatenate([cos_t, cos_t], axis=-1), jnp.concatenate([-sin_t, sin_t], axis=-1)


def clipped(raw):
    return jnp.minimum(jnp.maximum(raw.astype(jnp.float32), -CLIP_QKV), CLIP_QKV)


def rotate(vec, cos_t, sin_t):
    return (vec * cos_t + pltpu.roll(vec, HEAD_DIM // 2, 1) * sin_t).astype(jnp.bfloat16)


def unrotate(grad, cos_t, sin_t):
    grad = grad.astype(jnp.bfloat16).astype(jnp.float32)
    return grad * cos_t - pltpu.roll(grad, HEAD_DIM // 2, 1) * sin_t


def pass_clip(grad, raw):
    inside = jnp.abs(raw.astype(jnp.float32)) < CLIP_QKV
    return jnp.where(inside, grad, 0.0).astype(jnp.bfloat16)


def diagonal_mask():
    row = lax.broadcasted_iota(jnp.int32, (TILE_Q, TILE_Q), 0)
    col = lax.broadcasted_iota(jnp.int32, (TILE_Q, TILE_Q), 1)
    return row >= col


def mask_scores(scores, width, mask):
    tail = jnp.where(mask, scores[:, width - TILE_Q:], NEG_BIG)
    if width == TILE_Q:
        return tail
    return jnp.concatenate([scores[:, :width - TILE_Q], tail], axis=1)


def half_rows(own, size):
    side = lax.axis_index("tp") // 2
    start = side if own else 1 - side
    return pl.ds(pl.multiple_of(start * size, size), size)


def attn_fwd_kernel(groups, own_ref, far_ref, cos_ref, sin_ref, oown_ref, ofar_ref, lse_ref, qkv_ref, out_ref, k_scr, v_scr, s_scr, p_scr):
    half = own_ref.shape[0]
    own, far = half_rows(True, half), half_rows(False, half)
    qkv_ref[own, :] = own_ref[...]
    qkv_ref[far, :] = far_ref[...]
    seq_len = qkv_ref.shape[0]
    k_col = groups * HEAD_DIM
    k_scr[...] = rotate(clipped(qkv_ref[:, k_col:k_col + HEAD_DIM]), cos_ref[...], sin_ref[...])
    v_scr[...] = clipped(qkv_ref[:, k_col + HEAD_DIM:k_col + 2 * HEAD_DIM]).T.astype(jnp.bfloat16)
    row = lax.broadcasted_iota(jnp.int32, (TILE_Q, TILE_Q), 0)
    col = lax.broadcasted_iota(jnp.int32, (TILE_Q, TILE_Q), 1)
    mask = row <= col
    coef = HEAD_DIM ** -0.5 * LOG2E

    def head(g, carry):
        cols = pl.ds(pl.multiple_of(g * HEAD_DIM, HEAD_DIM), HEAD_DIM)

        def scored(qi):
            rows = slice(qi * TILE_Q, (qi + 1) * TILE_Q)
            query = rotate(clipped(qkv_ref[rows, cols]), cos_ref[rows, :], sin_ref[rows, :])
            peak = None
            for kj in range(qi + 1):
                keys = slice(kj * TILE_Q, (kj + 1) * TILE_Q)
                scores = dot(k_scr[keys, :], query, NT)
                if kj == qi:
                    scores = jnp.where(mask, scores, NEG_BIG)
                s_scr[qi % 2, keys, :] = scores
                part = jnp.max(scores.reshape(TILE_Q // 8, 8, TILE_Q), axis=0)
                peak = part if peak is None else jnp.maximum(peak, part)
            return jnp.max(peak, axis=0, keepdims=True) * coef

        def mixed(qi, shift):
            rows = slice(qi * TILE_Q, (qi + 1) * TILE_Q)
            total = None
            for kj in range(qi + 1):
                keys = slice(kj * TILE_Q, (kj + 1) * TILE_Q)
                prob = jnp.exp2(s_scr[qi % 2, keys, :] * coef - shift)
                p_scr[qi % 2, keys, :] = prob.astype(jnp.bfloat16)
                part = jnp.sum(prob.reshape(TILE_Q // 8, 8, TILE_Q), axis=0)
                total = part if total is None else total + part
            total = jnp.sum(total, axis=0, keepdims=True)
            out = dot(v_scr[:, :(qi + 1) * TILE_Q], p_scr[qi % 2, :(qi + 1) * TILE_Q, :], NN)
            out_ref[rows, cols] = (out * (1.0 / total)).T.astype(jnp.bfloat16)
            lse_ref[rows, cols] = jnp.broadcast_to(shift + jnp.log2(total), (HEAD_DIM, TILE_Q)).T

        tiles = seq_len // TILE_Q
        shift = scored(0)
        for qi in range(tiles):
            later = scored(qi + 1) if qi + 1 < tiles else None
            mixed(qi, shift)
            shift = later
        return carry

    lax.fori_loop(0, groups, head, 0)
    oown_ref[...] = out_ref[own, :]
    ofar_ref[...] = out_ref[far, :]


def attn_bwd_kernel(groups, own_ref, far_ref, aown_ref, afar_ref, down_ref, dfar_ref, lse_ref, cos_ref, sin_ref, gown_ref, gfar_ref, qkv_ref, attn_ref, dattn_ref, k_scr, v_scr, dk_scr, dv_scr):
    half = own_ref.shape[0]
    own, far = half_rows(True, half), half_rows(False, half)
    for dst, near, away in ((qkv_ref, own_ref, far_ref), (attn_ref, aown_ref, afar_ref), (dattn_ref, down_ref, dfar_ref)):
        dst[own, :] = near[...]
        dst[far, :] = away[...]
    seq_len = qkv_ref.shape[0]
    k_col = groups * HEAD_DIM
    v_col = k_col + HEAD_DIM
    scale = HEAD_DIM ** -0.5
    coef = scale * LOG2E
    k_scr[...] = rotate(clipped(qkv_ref[:, k_col:v_col]), cos_ref[...], sin_ref[...])
    v_scr[...] = clipped(qkv_ref[:, v_col:v_col + HEAD_DIM]).astype(jnp.bfloat16)
    dk_scr[...] = jnp.zeros_like(dk_scr)
    dv_scr[...] = jnp.zeros_like(dv_scr)
    mask = diagonal_mask()

    def head(g, carry):
        cols = pl.ds(pl.multiple_of(g * HEAD_DIM, HEAD_DIM), HEAD_DIM)
        for qi in range(seq_len // TILE_Q):
            rows = slice(qi * TILE_Q, (qi + 1) * TILE_Q)
            width = (qi + 1) * TILE_Q
            raw = qkv_ref[rows, cols]
            cos_t, sin_t = cos_ref[rows, :], sin_ref[rows, :]
            query = rotate(clipped(raw), cos_t, sin_t)
            dout = dattn_ref[rows, cols]
            delta = jnp.sum(dout.astype(jnp.float32) * attn_ref[rows, cols].astype(jnp.float32), axis=1, keepdims=True)
            scores = mask_scores(dot(query, k_scr[:width, :], NT), width, mask)
            lse = jnp.concatenate([lse_ref[rows, cols]] * (width // HEAD_DIM), axis=1)
            prob = jnp.exp2(scores * coef - lse)
            dprob = dot(dout, v_scr[:width, :], NT).astype(jnp.bfloat16).astype(jnp.float32)
            dscore = (prob * (dprob - delta)).astype(jnp.bfloat16)
            prob = prob.astype(jnp.bfloat16)
            dv_scr[:, :width] += dot(dout, prob, TN)
            dk_scr[:, :width] += dot(query, dscore, TN)
            dquery = dot(dscore, k_scr[:width, :], NN) * scale
            qkv_ref[rows, cols] = pass_clip(unrotate(dquery, cos_t, sin_t), raw)
        return carry

    lax.fori_loop(0, groups, head, 0)
    dkey = unrotate(dk_scr[...].T * scale, cos_ref[...], sin_ref[...])
    qkv_ref[:, k_col:v_col] = pass_clip(dkey, qkv_ref[:, k_col:v_col])
    qkv_ref[:, v_col:v_col + HEAD_DIM] = pass_clip(dv_scr[...].T, qkv_ref[:, v_col:v_col + HEAD_DIM])
    gown_ref[...] = qkv_ref[own, :]
    gfar_ref[...] = qkv_ref[far, :]


def head_specs(half, slot, wide):
    table = pl.BlockSpec((2 * half, HEAD_DIM), lambda n: (0, 0))
    part = pl.BlockSpec((half, wide), lambda n: (0, n))
    full = pl.BlockSpec((half, slot), lambda n: (0, n))
    lse = pl.BlockSpec((2 * half, wide), lambda n: (0, n))
    return table, part, full, lse


def attn_fwd(qkv_own, qkv_far, cos_t, sin_t, kv_loc):
    half = qkv_own.shape[0]
    slot = qkv_own.shape[1] // kv_loc
    groups = slot // HEAD_DIM - 2
    wide = groups * HEAD_DIM
    table, part, full, lse = head_specs(half, slot, wide)
    rows = jax.ShapeDtypeStruct((half, kv_loc * wide), jnp.bfloat16)
    return pl.pallas_call(
        functools.partial(attn_fwd_kernel, groups),
        grid=(kv_loc,),
        in_specs=[full, full, table, table],
        out_specs=[part, part, lse],
        out_shape=[rows, rows, jax.ShapeDtypeStruct((2 * half, kv_loc * wide), jnp.float32)],
        scratch_shapes=[pltpu.VMEM((2 * half, slot), jnp.bfloat16), pltpu.VMEM((2 * half, wide), jnp.bfloat16), pltpu.VMEM((2 * half, HEAD_DIM), jnp.bfloat16), pltpu.VMEM((HEAD_DIM, 2 * half), jnp.bfloat16), pltpu.VMEM((2, 2 * half, TILE_Q), jnp.float32), pltpu.VMEM((2, 2 * half, TILE_Q), jnp.bfloat16)],
        compiler_params=pltpu.CompilerParams(vmem_limit_bytes=48 * 2 ** 20),
        cost_estimate=pl.CostEstimate(flops=12 * 10 ** 9, bytes_accessed=14 * 10 ** 6, transcendentals=0),
        name="attn_fwd",
    )(qkv_own, qkv_far, cos_t, sin_t)


def attn_bwd(qkv_own, qkv_far, attn_own, attn_far, dattn_own, dattn_far, lse_t, cos_t, sin_t, kv_loc):
    half = qkv_own.shape[0]
    slot = qkv_own.shape[1] // kv_loc
    groups = slot // HEAD_DIM - 2
    wide = groups * HEAD_DIM
    table, part, full, lse = head_specs(half, slot, wide)
    return pl.pallas_call(
        functools.partial(attn_bwd_kernel, groups),
        grid=(kv_loc,),
        in_specs=[full, full, part, part, part, part, lse, table, table],
        out_specs=[full, full],
        out_shape=[jax.ShapeDtypeStruct(qkv_own.shape, jnp.bfloat16)] * 2,
        scratch_shapes=[pltpu.VMEM((2 * half, slot), jnp.bfloat16)] + [pltpu.VMEM((2 * half, wide), jnp.bfloat16)] * 2 + [pltpu.VMEM((2 * half, HEAD_DIM), jnp.bfloat16)] * 2 + [pltpu.VMEM((HEAD_DIM, 2 * half), jnp.float32)] * 2,
        compiler_params=pltpu.CompilerParams(vmem_limit_bytes=56 * 2 ** 20),
        cost_estimate=pl.CostEstimate(flops=25 * 10 ** 9, bytes_accessed=22 * 10 ** 6, transcendentals=0),
        name="attn_bwd",
    )(qkv_own, qkv_far, attn_own, attn_far, dattn_own, dattn_far, lse_t, cos_t, sin_t)


def dw_qkv_kernel(n_rows, *refs):
    acts, grads, out_ref = refs[:n_rows], refs[n_rows:-1], refs[-1]
    slot = out_ref.shape[2]
    for n in range(out_ref.shape[1]):
        cols = slice(n * slot, (n + 1) * slot)
        acc = sum(dot(a[...], g[:, cols], TN) for a, g in zip(acts, grads))
        out_ref[:, n, :] = acc.astype(jnp.bfloat16)


def dw_qkv(acts, grads, kv_loc, tile=512):
    rows, d_model = acts[0].shape
    width = grads[0].shape[1]
    slot = width // kv_loc
    whole = pl.BlockSpec((rows, width), lambda i: (0, 0))
    part = pl.BlockSpec((rows, tile), lambda i: (0, i))
    return pl.pallas_call(
        functools.partial(dw_qkv_kernel, len(acts)),
        grid=(d_model // tile,),
        in_specs=[part] * len(acts) + [whole] * len(grads),
        out_specs=pl.BlockSpec((tile, kv_loc, slot), lambda i: (i, 0, 0)),
        out_shape=jax.ShapeDtypeStruct((d_model, kv_loc, slot), jnp.bfloat16),
        compiler_params=pltpu.CompilerParams(vmem_limit_bytes=60 * 2 ** 20),
        cost_estimate=pl.CostEstimate(flops=51 * 10 ** 9, bytes_accessed=60 * 10 ** 6, transcendentals=0),
        name="dw_qkv",
    )(*acts, *grads)


def dw_out_kernel(n_rows, *refs):
    acts, grads, out_ref = refs[:n_rows], refs[n_rows:-1], refs[-1]
    out_ref[...] = sum(dot(a[...], g[...], TN) for a, g in zip(acts, grads)).astype(jnp.bfloat16)


def dw_out(acts, grads, tile=512):
    rows, width = acts[0].shape
    d_model = grads[0][1].shape[-1]
    whole = pl.BlockSpec((rows, width), lambda i: (0, 0))
    return pl.pallas_call(
        functools.partial(dw_out_kernel, len(acts)),
        grid=(d_model // tile,),
        in_specs=[whole] * len(acts) + [part_spec(g, b, (rows, tile), lambda i: (0, i)) for b, g in grads],
        out_specs=pl.BlockSpec((width, tile), lambda i: (0, i)),
        out_shape=jax.ShapeDtypeStruct((width, d_model), jnp.bfloat16),
        compiler_params=pltpu.CompilerParams(vmem_limit_bytes=60 * 2 ** 20),
        cost_estimate=pl.CostEstimate(flops=39 * 10 ** 9, bytes_accessed=50 * 10 ** 6, transcendentals=0),
        name="dw_out",
    )(*acts, *[g for _, g in grads])


def normalized(x_f32):
    centered = x_f32 - jnp.mean(x_f32, axis=-1, keepdims=True)
    rstd = lax.rsqrt(jnp.mean(centered * centered, axis=-1, keepdims=True) + LN_EPS)
    return centered * rstd, rstd


def norm_fwd_kernel(x_ref, gain_ref, h_ref):
    hat, _ = normalized(x_ref[0].astype(jnp.float32))
    h_ref[...] = (hat * gain_ref[...].astype(jnp.float32)).astype(jnp.bfloat16)


def norm_fwd(x_seq, gain, b, tile=64):
    _, rows, d_model = x_seq.shape
    return pl.pallas_call(
        norm_fwd_kernel,
        grid=(rows // tile,),
        in_specs=[pl.BlockSpec((1, tile, d_model), lambda i: (b, i, 0)), pl.BlockSpec((1, d_model), lambda i: (0, 0))],
        out_specs=pl.BlockSpec((tile, d_model), lambda i: (i, 0)),
        out_shape=jax.ShapeDtypeStruct((rows, d_model), jnp.bfloat16),
        cost_estimate=pl.CostEstimate(flops=2 * 10 ** 9, bytes_accessed=7 * 10 ** 6, transcendentals=0),
        name="norm_fwd",
    )(x_seq, gain)


def residual_kernel(x_ref, near_ref, far_ref, *rest):
    total = near_ref[...].astype(jnp.float32) + far_ref[...].astype(jnp.float32)
    rest[-1][0] = (x_ref[0].astype(jnp.float32) + total.astype(jnp.bfloat16).astype(jnp.float32)).astype(jnp.bfloat16)


def norm_bwd_kernel(x_ref, dy_ref, gain_ref, near_ref, far_ref, *rest):
    dx_ref, dgain_ref, sum_ref = rest[-3:]

    @pl.when(pl.program_id(0) == 0)
    def _():
        sum_ref[...] = jnp.zeros_like(sum_ref)

    def group(i, carry):
        rows = pl.ds(pl.multiple_of(i * 16, 16), 16)
        hat, rstd = normalized(x_ref[0, rows, :].astype(jnp.float32))
        dh = (near_ref[rows, :].astype(jnp.float32) + far_ref[rows, :].astype(jnp.float32)).astype(jnp.bfloat16).astype(jnp.float32)
        prod = dh * hat
        sum_ref[...] += prod[:8] + prod[8:]
        dhat = dh * gain_ref[...].astype(jnp.float32)
        inner = dhat - jnp.mean(dhat, axis=-1, keepdims=True) - hat * jnp.mean(dhat * hat, axis=-1, keepdims=True)
        dx_ref[0, rows, :] = (dy_ref[0, rows, :].astype(jnp.float32) + inner * rstd).astype(jnp.bfloat16)
        return carry

    lax.fori_loop(0, x_ref.shape[1] // 16, group, 0, unroll=2)

    @pl.when(pl.program_id(0) == pl.num_programs(0) - 1)
    def _():
        dgain_ref[...] = jnp.sum(sum_ref[...], axis=0, keepdims=True)


def residual(x_seq, near, far, b, held, tile=64):
    _, rows, d_model = x_seq.shape
    whole = pl.BlockSpec((1, tile, d_model), lambda i: (b, i, 0))
    part = pl.BlockSpec((tile, d_model), lambda i: (i, 0))
    keep = [] if held is None else [held]
    return pl.pallas_call(
        residual_kernel,
        grid=(rows // tile,),
        in_specs=[whole, part, part] + [pl.BlockSpec(memory_space=pl.ANY)] * len(keep),
        out_specs=whole,
        out_shape=jax.ShapeDtypeStruct(x_seq.shape, jnp.bfloat16),
        input_output_aliases={3: 0} if keep else {},
        cost_estimate=pl.CostEstimate(flops=2 * 10 ** 9, bytes_accessed=13 * 10 ** 6, transcendentals=0),
        name="residual",
    )(x_seq, near, far, *keep)


def norm_bwd(x_seq, y_grad, gain, near, far, b, base, held, tile=64):
    _, _, d_model = x_seq.shape
    first = base // tile
    whole = pl.BlockSpec((1, tile, d_model), lambda i: (b, first + i, 0))
    part = pl.BlockSpec((tile, d_model), lambda i: (first + i, 0))
    piece = pl.BlockSpec((tile, d_model), lambda i: (i, 0))
    row = pl.BlockSpec((1, d_model), lambda i: (0, 0))
    keep = [] if held is None else [held]
    return pl.pallas_call(
        norm_bwd_kernel,
        grid=(far.shape[0] // tile,),
        in_specs=[whole, whole, row, part, piece] + [pl.BlockSpec(memory_space=pl.ANY)] * len(keep),
        out_specs=[whole, row],
        out_shape=[jax.ShapeDtypeStruct(x_seq.shape, jnp.bfloat16), jax.ShapeDtypeStruct((1, d_model), jnp.float32)],
        input_output_aliases={5: 0} if keep else {},
        scratch_shapes=[pltpu.VMEM((8, d_model), jnp.float32)],
        cost_estimate=pl.CostEstimate(flops=4 * 10 ** 9, bytes_accessed=16 * 10 ** 6, transcendentals=0),
        name="norm_bwd",
    )(x_seq, y_grad, gain, near, far, *keep)


def proj_deep_kernel(n_parts, dims, *refs):
    parts, w_ref, outs, accs = refs[:n_parts], refs[n_parts], refs[n_parts + 1:2 * n_parts + 1], refs[2 * n_parts + 1:]
    step, last = pl.program_id(0), pl.num_programs(0) - 1

    @pl.when(step == 0)
    def _():
        for a, acc in zip(parts, accs):
            acc[...] = dot(a[...], w_ref[...], dims)

    @pl.when((step > 0) & (step < last))
    def _():
        for a, acc in zip(parts, accs):
            acc[...] += dot(a[...], w_ref[...], dims)

    @pl.when(step == last)
    def _():
        for a, acc, out in zip(parts, accs, outs):
            out[...] = (acc[...] + dot(a[...], w_ref[...], dims)).astype(jnp.bfloat16)


def part_spec(a, b, block, index):
    if a.ndim == 2:
        return pl.BlockSpec(block, index)
    return pl.BlockSpec((None,) + block, lambda i: (b,) + index(i))


def proj_deep(parts, w, dims, tile=1024):
    rows, depth = parts[0].shape[-2:]
    width = w.shape[0] if dims is NT else w.shape[1]
    w_spec = pl.BlockSpec((width, tile), lambda i: (0, i)) if dims is NT else pl.BlockSpec((tile, width), lambda i: (i, 0))
    return pl.pallas_call(
        functools.partial(proj_deep_kernel, len(parts), dims),
        grid=(depth // tile,),
        in_specs=[part_spec(a, b, (rows, tile), lambda i: (0, i)) for b, a in enumerate(parts)] + [w_spec],
        out_specs=[pl.BlockSpec((rows, width), lambda i: (0, 0))] * len(parts),
        out_shape=[jax.ShapeDtypeStruct((rows, width), jnp.bfloat16)] * len(parts),
        scratch_shapes=[pltpu.VMEM((rows, width), jnp.float32)] * len(parts),
        compiler_params=pltpu.CompilerParams(vmem_limit_bytes=60 * 2 ** 20),
        cost_estimate=pl.CostEstimate(flops=2 * len(parts) * rows * depth * width, bytes_accessed=2 * depth * width, transcendentals=0),
        name="proj_deep",
    )(*parts, w)


def proj_wide_kernel(n_parts, dims, *refs):
    w_ref = refs[n_parts]
    for a, out in zip(refs[:n_parts], refs[n_parts + 1:]):
        out[...] = dot(a[...], w_ref[...], dims).astype(jnp.bfloat16)


def proj_wide(parts, w, dims, tile=1024):
    rows, depth = parts[0].shape
    width = w.shape[0] if dims is NT else w.shape[1]
    w_spec = pl.BlockSpec((tile, depth), lambda i: (i, 0)) if dims is NT else pl.BlockSpec((depth, tile), lambda i: (0, i))
    return pl.pallas_call(
        functools.partial(proj_wide_kernel, len(parts), dims),
        grid=(width // tile,),
        in_specs=[pl.BlockSpec((rows, depth), lambda i: (0, 0))] * len(parts) + [w_spec],
        out_specs=[pl.BlockSpec((rows, tile), lambda i: (0, i))] * len(parts),
        out_shape=[jax.ShapeDtypeStruct((rows, width), jnp.bfloat16)] * len(parts),
        compiler_params=pltpu.CompilerParams(vmem_limit_bytes=60 * 2 ** 20),
        cost_estimate=pl.CostEstimate(flops=2 * len(parts) * rows * depth * width, bytes_accessed=2 * depth * width, transcendentals=0),
        name="proj_wide",
    )(*parts, w)


def solution(mesh):
    n_tp = mesh.shape["tp"]
    pairs = [[i, i + 1] for i in range(0, n_tp, 2)]

    def swap(value, bit):
        return lax.ppermute(value, "tp", [(i, i ^ bit) for i in range(n_tp)])

    def pair_gather(value, axis=0):
        return lax.all_gather(value, "tp", axis_index_groups=pairs, axis=axis, tiled=True)

    def pair_scatter(value):
        return lax.psum_scatter(value, "tp", axis_index_groups=pairs, scatter_dimension=0, tiled=True)

    def staged_step(x_seq, ln_gain, w_qkv, w_out, y_grad):
        kv_loc = w_qkv.shape[1]
        gain = ln_gain[None, :]
        token = [None]

        def run(fn, lead, *rest):
            if token[0] is not None:
                lead, _ = lax.optimization_barrier((lead, token[0]))
            result = fn(lead, *rest)
            token[0] = jax.tree.leaves(result)[0]
            return result

        cos_t, sin_t = rope_tables(x_seq.shape[1] * n_tp)
        h0 = run(lambda x: norm_fwd(x, gain, 0), x_seq)
        hx0 = swap(h0, 2)
        h1 = run(lambda x: norm_fwd(x, gain, 1), x_seq)
        hx1 = swap(h1, 2)
        dy0, dy1, _ = lax.optimization_barrier((y_grad[0], y_grad[1], h1))
        dyx0 = swap(dy0, 2)
        dyx1 = swap(dy1, 2)
        h_own0, h_own1 = pair_gather(h0), pair_gather(h1)
        dy_own = pair_gather(y_grad, 1)
        w_flat = run(lambda w: lax.optimization_barrier(w.reshape(w.shape[0], -1)), w_qkv)
        qkv_own0, qkv_own1 = run(lambda h: proj_deep([h, h_own1], w_flat, NN), h_own0)
        h_far0 = pair_gather(hx0)
        dattn_own0, dattn_own1 = run(lambda d: proj_deep([d, d], w_out, NT), dy_own)
        (qkv_far0,) = run(lambda h: proj_deep([h], w_flat, NN), h_far0)
        attn_own0, attn_far0, lse0 = run(lambda far: attn_fwd(qkv_own0, far, cos_t, sin_t, kv_loc), qkv_far0)
        h_far1 = pair_gather(hx1)
        o_far0, o_near0 = run(lambda a: proj_wide([a, attn_own0], w_out, NN), attn_far0)
        os_far0, os_near0 = pair_scatter(o_far0), pair_scatter(o_near0)
        (qkv_far1,) = run(lambda h: proj_deep([h], w_flat, NN), h_far1)
        ox0 = swap(os_far0, 2)
        attn_own1, attn_far1, lse1 = run(lambda far: attn_fwd(qkv_own1, far, cos_t, sin_t, kv_loc), qkv_far1)
        dy_far0 = pair_gather(dyx0)
        o_far1, o_near1 = run(lambda a: proj_wide([a, attn_own1], w_out, NN), attn_far1)
        os_far1, os_near1 = pair_scatter(o_far1), pair_scatter(o_near1)
        (dattn_far0,) = run(lambda d: proj_deep([d], w_out, NT), dy_far0)
        ox1 = swap(os_far1, 2)
        dq_own0, dq_far0 = run(lambda d: attn_bwd(qkv_own0, qkv_far0, attn_own0, attn_far0, dattn_own0, d, lse0, cos_t, sin_t, kv_loc), dattn_far0)
        dy_far1 = pair_gather(dyx1)
        dh_far0, dh_near0 = run(lambda d: proj_wide([d, dq_own0], w_flat, NT), dq_far0)
        dhs_far0, dhs_near0 = pair_scatter(dh_far0), pair_scatter(dh_near0)
        (dattn_far1,) = run(lambda d: proj_deep([d], w_out, NT), dy_far1)
        dhx0 = swap(dhs_far0, 2)
        dq_own1, dq_far1 = run(lambda d: attn_bwd(qkv_own1, qkv_far1, attn_own1, attn_far1, dattn_own1, d, lse1, cos_t, sin_t, kv_loc), dattn_far1)
        dh_far1, dh_near1 = run(lambda d: proj_wide([d, dq_own1], w_flat, NT), dq_far1)
        dhs_far1, dhs_near1 = pair_scatter(dh_far1), pair_scatter(dh_near1)
        wout_grad = run(lambda a: dw_out([a, attn_far0, attn_own1, attn_far1], [(0, dy_own), (0, dy_far0), (1, dy_own), (0, dy_far1)]), attn_own0)
        cut = dhs_far1.shape[0] // 2
        dhx1a, dhx1b = swap(dhs_far1[:cut], 2), swap(dhs_far1[cut:], 2)
        y_out = run(lambda near: residual(x_seq, near, ox0, 0, None), os_near0)
        y_out = run(lambda near: residual(x_seq, near, ox1, 1, y_out), os_near1)
        wqkv_grad = run(lambda h: dw_qkv([h, h_far0, h_own1, h_far1], [dq_own0, dq_far0, dq_own1, dq_far1], kv_loc), h_own0)
        x_grad, gain0 = run(lambda near: norm_bwd(x_seq, y_grad, gain, near, dhx0, 0, 0, None), dhs_near0)
        x_grad, gain1 = run(lambda near: norm_bwd(x_seq, y_grad, gain, near, dhx1a, 1, 0, x_grad), dhs_near1)
        x_grad, gain2 = run(lambda near: norm_bwd(x_seq, y_grad, gain, near, dhx1b, 1, cut, x_grad), dhs_near1)
        mine = gain0 + gain1 + gain2
        gain_grad = (mine + swap(mine, 1) + swap(mine, 2) + swap(mine, 3)).astype(jnp.bfloat16)[0]
        return y_out, x_grad, gain_grad, wqkv_grad, wout_grad

    specs_in = (P('dp', 'tp', None), P(None), P(None, 'tp', None), P('tp', None), P('dp', 'tp', None))
    specs_out = (P('dp', 'tp', None), P('dp', 'tp', None), P('dp'), P('dp', 'tp', None), P(('dp', 'tp'), None))
    return jax.shard_map(staged_step, mesh=mesh, in_specs=specs_in, out_specs=specs_out, check_vma=False)
```

```python
import functools
import jax
import jax.numpy as jnp
from jax import lax
from jax.experimental import pallas as pl
from jax.experimental.pallas import tpu as pltpu
from jax.sharding import PartitionSpec as P

CLIP_QKV = 8.0
ROPE_THETA = 500000.0
LN_EPS = 1e-5
LOG2E = 1.4426950408889634
HEAD_DIM = 128
TILE_Q = 256
NEG_BIG = -1e30
NT = (((1,), (1,)), ((), ()))
TN = (((0,), (0,)), ((), ()))
NN = (((1,), (0,)), ((), ()))


def dot(a, b, dims):
    return lax.dot_general(a, b, dims, preferred_element_type=jnp.float32)


def rope_tables(seq_len):
    inv_freq = 1.0 / (ROPE_THETA ** (jnp.arange(0, HEAD_DIM, 2, dtype=jnp.float32) / HEAD_DIM))
    angles = jnp.arange(seq_len, dtype=jnp.float32)[:, None] * inv_freq[None, :]
    cos_t, sin_t = jnp.cos(angles), jnp.sin(angles)
    return jnp.concatenate([cos_t, cos_t], axis=-1), jnp.concatenate([-sin_t, sin_t], axis=-1)


def clipped(raw):
    return jnp.minimum(jnp.maximum(raw.astype(jnp.float32), -CLIP_QKV), CLIP_QKV)


def rotate(vec, cos_t, sin_t):
    return (vec * cos_t + pltpu.roll(vec, HEAD_DIM // 2, 1) * sin_t).astype(jnp.bfloat16)


def unrotate(grad, cos_t, sin_t):
    grad = grad.astype(jnp.bfloat16).astype(jnp.float32)
    return grad * cos_t - pltpu.roll(grad, HEAD_DIM // 2, 1) * sin_t


def pass_clip(grad, raw):
    inside = jnp.abs(raw.astype(jnp.float32)) < CLIP_QKV
    return jnp.where(inside, grad, 0.0).astype(jnp.bfloat16)


def diagonal_mask():
    row = lax.broadcasted_iota(jnp.int32, (TILE_Q, TILE_Q), 0)
    col = lax.broadcasted_iota(jnp.int32, (TILE_Q, TILE_Q), 1)
    return row >= col


def half_rows(own, size):
    side = lax.axis_index("tp") // 2
    start = side if own else 1 - side
    return pl.ds(pl.multiple_of(start * size, size), size)


def attn_fwd_kernel(groups, own_ref, far_ref, cos_ref, sin_ref, oown_ref, ofar_ref, lse_ref, qkv_ref, out_ref, k_scr, v_scr, s_scr, p_scr):
    half = own_ref.shape[0]
    own, far = half_rows(True, half), half_rows(False, half)
    qkv_ref[own, :] = own_ref[...]
    qkv_ref[far, :] = far_ref[...]
    seq_len = qkv_ref.shape[0]
    k_col = groups * HEAD_DIM
    k_scr[...] = rotate(clipped(qkv_ref[:, k_col:k_col + HEAD_DIM]), cos_ref[...], sin_ref[...])
    v_scr[...] = clipped(qkv_ref[:, k_col + HEAD_DIM:k_col + 2 * HEAD_DIM]).T.astype(jnp.bfloat16)
    row = lax.broadcasted_iota(jnp.int32, (TILE_Q, TILE_Q), 0)
    col = lax.broadcasted_iota(jnp.int32, (TILE_Q, TILE_Q), 1)
    mask = row <= col
    coef = HEAD_DIM ** -0.5 * LOG2E

    def head(g, carry):
        cols = pl.ds(pl.multiple_of(g * HEAD_DIM, HEAD_DIM), HEAD_DIM)

        def scored(qi):
            rows = slice(qi * TILE_Q, (qi + 1) * TILE_Q)
            query = rotate(clipped(qkv_ref[rows, cols]), cos_ref[rows, :], sin_ref[rows, :])
            peak = None
            for kj in range(qi + 1):
                keys = slice(kj * TILE_Q, (kj + 1) * TILE_Q)
                scores = dot(k_scr[keys, :], query, NT)
                if kj == qi:
                    scores = jnp.where(mask, scores, NEG_BIG)
                s_scr[qi % 2, keys, :] = scores
                part = jnp.max(scores.reshape(TILE_Q // 8, 8, TILE_Q), axis=0)
                peak = part if peak is None else jnp.maximum(peak, part)
            return jnp.max(peak, axis=0, keepdims=True) * coef

        def mixed(qi, shift):
            rows = slice(qi * TILE_Q, (qi + 1) * TILE_Q)
            total = None
            for kj in range(qi + 1):
                keys = slice(kj * TILE_Q, (kj + 1) * TILE_Q)
                prob = jnp.exp2(s_scr[qi % 2, keys, :] * coef - shift)
                p_scr[qi % 2, keys, :] = prob.astype(jnp.bfloat16)
                part = jnp.sum(prob.reshape(TILE_Q // 8, 8, TILE_Q), axis=0)
                total = part if total is None else total + part
            total = jnp.sum(total, axis=0, keepdims=True)
            out = dot(v_scr[:, :(qi + 1) * TILE_Q], p_scr[qi % 2, :(qi + 1) * TILE_Q, :], NN)
            out_ref[rows, cols] = (out * (1.0 / total)).T.astype(jnp.bfloat16)
            lse_ref[rows, cols] = jnp.broadcast_to(shift + jnp.log2(total), (HEAD_DIM, TILE_Q)).T

        tiles = seq_len // TILE_Q
        shift = scored(0)
        for qi in range(tiles):
            later = scored(qi + 1) if qi + 1 < tiles else None
            mixed(qi, shift)
            shift = later
        return carry

    lax.fori_loop(0, groups, head, 0)
    oown_ref[...] = out_ref[own, :]
    ofar_ref[...] = out_ref[far, :]


def attn_bwd_kernel(groups, own_ref, far_ref, aown_ref, afar_ref, down_ref, dfar_ref, lse_ref, cos_ref, sin_ref, gown_ref, gfar_ref, qkv_ref, attn_ref, dattn_ref, k_scr, v_scr, dk_scr, dv_scr, q_scr, p_scr, s_scr):
    half = own_ref.shape[0]
    own, far = half_rows(True, half), half_rows(False, half)
    for dst, near, away in ((qkv_ref, own_ref, far_ref), (attn_ref, aown_ref, afar_ref), (dattn_ref, down_ref, dfar_ref)):
        dst[own, :] = near[...]
        dst[far, :] = away[...]
    seq_len = qkv_ref.shape[0]
    k_col = groups * HEAD_DIM
    v_col = k_col + HEAD_DIM
    scale = HEAD_DIM ** -0.5
    coef = scale * LOG2E
    k_scr[...] = rotate(clipped(qkv_ref[:, k_col:v_col]), cos_ref[...], sin_ref[...])
    v_scr[...] = clipped(qkv_ref[:, v_col:v_col + HEAD_DIM]).astype(jnp.bfloat16)
    dk_scr[...] = jnp.zeros_like(dk_scr)
    dv_scr[...] = jnp.zeros_like(dv_scr)
    mask = diagonal_mask()

    def head(g, carry):
        cols = pl.ds(pl.multiple_of(g * HEAD_DIM, HEAD_DIM), HEAD_DIM)

        def scored(qi):
            rows = slice(qi * TILE_Q, (qi + 1) * TILE_Q)
            query = rotate(clipped(qkv_ref[rows, cols]), cos_ref[rows, :], sin_ref[rows, :])
            q_scr[qi % 2] = query
            dout = dattn_ref[rows, cols]
            delta = jnp.sum(dout.astype(jnp.float32) * attn_ref[rows, cols].astype(jnp.float32), axis=1, keepdims=True)
            lse = jnp.concatenate([lse_ref[rows, cols]] * (TILE_Q // HEAD_DIM), axis=1)
            for kj in range(qi + 1):
                keys = slice(kj * TILE_Q, (kj + 1) * TILE_Q)
                scores = dot(query, k_scr[keys, :], NT)
                if kj == qi:
                    scores = jnp.where(mask, scores, NEG_BIG)
                prob = jnp.exp2(scores * coef - lse)
                dprob = dot(dout, v_scr[keys, :], NT).astype(jnp.bfloat16).astype(jnp.float32)
                p_scr[qi % 2, :, keys] = prob.astype(jnp.bfloat16)
                s_scr[qi % 2, :, keys] = (prob * (dprob - delta)).astype(jnp.bfloat16)

        def mixed(qi):
            rows = slice(qi * TILE_Q, (qi + 1) * TILE_Q)
            width = (qi + 1) * TILE_Q
            dscore = s_scr[qi % 2, :, :width]
            dv_scr[:, :width] += dot(dattn_ref[rows, cols], p_scr[qi % 2, :, :width], TN)
            dk_scr[:, :width] += dot(q_scr[qi % 2], dscore, TN)
            dquery = dot(dscore, k_scr[:width, :], NN) * scale
            qkv_ref[rows, cols] = pass_clip(unrotate(dquery, cos_ref[rows, :], sin_ref[rows, :]), qkv_ref[rows, cols])

        tiles = seq_len // TILE_Q
        scored(0)
        for qi in range(tiles):
            if qi + 1 < tiles:
                scored(qi + 1)
            mixed(qi)
        return carry

    lax.fori_loop(0, groups, head, 0)
    dkey = unrotate(dk_scr[...].T * scale, cos_ref[...], sin_ref[...])
    qkv_ref[:, k_col:v_col] = pass_clip(dkey, qkv_ref[:, k_col:v_col])
    qkv_ref[:, v_col:v_col + HEAD_DIM] = pass_clip(dv_scr[...].T, qkv_ref[:, v_col:v_col + HEAD_DIM])
    gown_ref[...] = qkv_ref[own, :]
    gfar_ref[...] = qkv_ref[far, :]


def head_specs(half, slot, wide):
    table = pl.BlockSpec((2 * half, HEAD_DIM), lambda n: (0, 0))
    part = pl.BlockSpec((half, wide), lambda n: (0, n))
    full = pl.BlockSpec((half, slot), lambda n: (0, n))
    lse = pl.BlockSpec((2 * half, wide), lambda n: (0, n))
    return table, part, full, lse


def attn_fwd(qkv_own, qkv_far, cos_t, sin_t, kv_loc):
    half = qkv_own.shape[0]
    slot = qkv_own.shape[1] // kv_loc
    groups = slot // HEAD_DIM - 2
    wide = groups * HEAD_DIM
    table, part, full, lse = head_specs(half, slot, wide)
    rows = jax.ShapeDtypeStruct((half, kv_loc * wide), jnp.bfloat16)
    return pl.pallas_call(
        functools.partial(attn_fwd_kernel, groups),
        grid=(kv_loc,),
        in_specs=[full, full, table, table],
        out_specs=[part, part, lse],
        out_shape=[rows, rows, jax.ShapeDtypeStruct((2 * half, kv_loc * wide), jnp.float32)],
        scratch_shapes=[pltpu.VMEM((2 * half, slot), jnp.bfloat16), pltpu.VMEM((2 * half, wide), jnp.bfloat16), pltpu.VMEM((2 * half, HEAD_DIM), jnp.bfloat16), pltpu.VMEM((HEAD_DIM, 2 * half), jnp.bfloat16), pltpu.VMEM((2, 2 * half, TILE_Q), jnp.float32), pltpu.VMEM((2, 2 * half, TILE_Q), jnp.bfloat16)],
        compiler_params=pltpu.CompilerParams(vmem_limit_bytes=62 * 2 ** 20),
        cost_estimate=pl.CostEstimate(flops=12 * 10 ** 9, bytes_accessed=14 * 10 ** 6, transcendentals=0),
        name="attn_fwd",
    )(qkv_own, qkv_far, cos_t, sin_t)


def attn_bwd(qkv_own, qkv_far, attn_own, attn_far, dattn_own, dattn_far, lse_t, cos_t, sin_t, kv_loc):
    half = qkv_own.shape[0]
    slot = qkv_own.shape[1] // kv_loc
    groups = slot // HEAD_DIM - 2
    wide = groups * HEAD_DIM
    table, part, full, lse = head_specs(half, slot, wide)
    return pl.pallas_call(
        functools.partial(attn_bwd_kernel, groups),
        grid=(kv_loc,),
        in_specs=[full, full, part, part, part, part, lse, table, table],
        out_specs=[full, full],
        out_shape=[jax.ShapeDtypeStruct(qkv_own.shape, jnp.bfloat16)] * 2,
        scratch_shapes=[pltpu.VMEM((2 * half, slot), jnp.bfloat16)] + [pltpu.VMEM((2 * half, wide), jnp.bfloat16)] * 2 + [pltpu.VMEM((2 * half, HEAD_DIM), jnp.bfloat16)] * 2 + [pltpu.VMEM((HEAD_DIM, 2 * half), jnp.float32)] * 2 + [pltpu.VMEM((2, TILE_Q, HEAD_DIM), jnp.bfloat16)] + [pltpu.VMEM((2, TILE_Q, 2 * half), jnp.bfloat16)] * 2,
        compiler_params=pltpu.CompilerParams(vmem_limit_bytes=62 * 2 ** 20),
        cost_estimate=pl.CostEstimate(flops=25 * 10 ** 9, bytes_accessed=22 * 10 ** 6, transcendentals=0),
        name="attn_bwd",
    )(qkv_own, qkv_far, attn_own, attn_far, dattn_own, dattn_far, lse_t, cos_t, sin_t)


def dw_qkv_kernel(n_rows, *refs):
    acts, grads, out_ref = refs[:n_rows], refs[n_rows:-1], refs[-1]
    slot = out_ref.shape[2]
    for n in range(out_ref.shape[1]):
        cols = slice(n * slot, (n + 1) * slot)
        acc = sum(dot(a[...], g[:, cols], TN) for a, g in zip(acts, grads))
        out_ref[:, n, :] = acc.astype(jnp.bfloat16)


def dw_qkv(acts, grads, kv_loc, tile=512):
    rows, d_model = acts[0].shape
    width = grads[0].shape[1]
    slot = width // kv_loc
    whole = pl.BlockSpec((rows, width), lambda i: (0, 0))
    part = pl.BlockSpec((rows, tile), lambda i: (0, i))
    return pl.pallas_call(
        functools.partial(dw_qkv_kernel, len(acts)),
        grid=(d_model // tile,),
        in_specs=[part] * len(acts) + [whole] * len(grads),
        out_specs=pl.BlockSpec((tile, kv_loc, slot), lambda i: (i, 0, 0)),
        out_shape=jax.ShapeDtypeStruct((d_model, kv_loc, slot), jnp.bfloat16),
        compiler_params=pltpu.CompilerParams(vmem_limit_bytes=62 * 2 ** 20),
        cost_estimate=pl.CostEstimate(flops=51 * 10 ** 9, bytes_accessed=60 * 10 ** 6, transcendentals=0),
        name="dw_qkv",
    )(*acts, *grads)


def dw_out_kernel(n_rows, *refs):
    acts, grads, out_ref = refs[:n_rows], refs[n_rows:-1], refs[-1]
    out_ref[...] = sum(dot(a[...], g[...], TN) for a, g in zip(acts, grads)).astype(jnp.bfloat16)


def dw_out(acts, grads, tile=512):
    rows, width = acts[0].shape
    d_model = grads[0][1].shape[-1]
    whole = pl.BlockSpec((rows, width), lambda i: (0, 0))
    return pl.pallas_call(
        functools.partial(dw_out_kernel, len(acts)),
        grid=(d_model // tile,),
        in_specs=[whole] * len(acts) + [part_spec(g, b, (rows, tile), lambda i: (0, i)) for b, g in grads],
        out_specs=pl.BlockSpec((width, tile), lambda i: (0, i)),
        out_shape=jax.ShapeDtypeStruct((width, d_model), jnp.bfloat16),
        compiler_params=pltpu.CompilerParams(vmem_limit_bytes=62 * 2 ** 20),
        cost_estimate=pl.CostEstimate(flops=39 * 10 ** 9, bytes_accessed=50 * 10 ** 6, transcendentals=0),
        name="dw_out",
    )(*acts, *[g for _, g in grads])


def norm_fwd_kernel(x_ref, gain_ref, h_ref, stat_ref):
    def group(i, carry):
        rows = pl.ds(pl.multiple_of(i * 16, 16), 16)
        x_f32 = x_ref[0, rows, :].astype(jnp.float32)
        mean = jnp.mean(x_f32, axis=-1, keepdims=True)
        centered = x_f32 - mean
        rstd = lax.rsqrt(jnp.mean(centered * centered, axis=-1, keepdims=True) + LN_EPS)
        h_ref[rows, :] = (centered * rstd * gain_ref[...].astype(jnp.float32)).astype(jnp.bfloat16)
        stat_ref[rows, :HEAD_DIM] = jnp.broadcast_to(mean, (16, HEAD_DIM))
        stat_ref[rows, HEAD_DIM:] = jnp.broadcast_to(rstd, (16, HEAD_DIM))
        return carry

    lax.fori_loop(0, x_ref.shape[1] // 16, group, 0, unroll=2)


def norm_fwd(x_seq, gain, b, tile=64):
    _, rows, d_model = x_seq.shape
    return pl.pallas_call(
        norm_fwd_kernel,
        grid=(rows // tile,),
        in_specs=[pl.BlockSpec((1, tile, d_model), lambda i: (b, i, 0)), pl.BlockSpec((1, d_model), lambda i: (0, 0))],
        out_specs=[pl.BlockSpec((tile, d_model), lambda i: (i, 0)), pl.BlockSpec((tile, 2 * HEAD_DIM), lambda i: (i, 0))],
        out_shape=[jax.ShapeDtypeStruct((rows, d_model), jnp.bfloat16), jax.ShapeDtypeStruct((rows, 2 * HEAD_DIM), jnp.float32)],
        compiler_params=pltpu.CompilerParams(vmem_limit_bytes=62 * 2 ** 20),
        cost_estimate=pl.CostEstimate(flops=2 * 10 ** 9, bytes_accessed=7 * 10 ** 6, transcendentals=0),
        name="norm_fwd",
    )(x_seq, gain)


def residual_kernel(x_ref, near0_ref, near1_ref, far0_ref, far1_ref, out_ref):
    for b, (near, far) in enumerate(((near0_ref, far0_ref), (near1_ref, far1_ref))):
        total = (near[...].astype(jnp.float32) + far[...].astype(jnp.float32)).astype(jnp.bfloat16)
        out_ref[b] = (x_ref[b].astype(jnp.float32) + total.astype(jnp.float32)).astype(jnp.bfloat16)


def norm_bwd_kernel(x_ref, dy_ref, gain_ref, near_ref, far_ref, stat_ref, *rest):
    dx_ref, dgain_ref, sum_ref = rest[-3:]

    @pl.when(pl.program_id(0) == 0)
    def _():
        sum_ref[...] = jnp.zeros_like(sum_ref)

    def group(i, carry):
        rows = pl.ds(pl.multiple_of(i * 16, 16), 16)
        mean, rstd = stat_ref[rows, :1], stat_ref[rows, HEAD_DIM:HEAD_DIM + 1]
        hat = (x_ref[0, rows, :].astype(jnp.float32) - mean) * rstd
        dh = (near_ref[rows, :].astype(jnp.float32) + far_ref[rows, :].astype(jnp.float32)).astype(jnp.bfloat16).astype(jnp.float32)
        prod = dh * hat
        sum_ref[...] += prod[:8] + prod[8:]
        dhat = dh * gain_ref[...].astype(jnp.float32)
        inner = dhat - jnp.mean(dhat, axis=-1, keepdims=True) - hat * jnp.mean(dhat * hat, axis=-1, keepdims=True)
        dx_ref[0, rows, :] = (dy_ref[0, rows, :].astype(jnp.float32) + inner * rstd).astype(jnp.bfloat16)
        return carry

    lax.fori_loop(0, x_ref.shape[1] // 16, group, 0, unroll=2)

    @pl.when(pl.program_id(0) == pl.num_programs(0) - 1)
    def _():
        dgain_ref[...] = jnp.sum(sum_ref[...], axis=0, keepdims=True)


def residual(x_seq, nears, fars, tile=64):
    batch, rows, d_model = x_seq.shape
    whole = pl.BlockSpec((batch, tile, d_model), lambda i: (0, i, 0))
    part = pl.BlockSpec((tile, d_model), lambda i: (i, 0))
    return pl.pallas_call(
        residual_kernel,
        grid=(rows // tile,),
        in_specs=[whole] + [part] * 4,
        out_specs=whole,
        out_shape=jax.ShapeDtypeStruct(x_seq.shape, jnp.bfloat16),
        compiler_params=pltpu.CompilerParams(vmem_limit_bytes=62 * 2 ** 20),
        cost_estimate=pl.CostEstimate(flops=4 * 10 ** 9, bytes_accessed=26 * 10 ** 6, transcendentals=0),
        name="residual",
    )(x_seq, *nears, *fars)


def norm_bwd(x_seq, y_grad, gain, near, far, stat, b, base, held, tile=64):
    _, _, d_model = x_seq.shape
    first = base // tile
    whole = pl.BlockSpec((1, tile, d_model), lambda i: (b, first + i, 0))
    part = pl.BlockSpec((tile, d_model), lambda i: (first + i, 0))
    piece = pl.BlockSpec((tile, d_model), lambda i: (i, 0))
    row = pl.BlockSpec((1, d_model), lambda i: (0, 0))
    keep = [] if held is None else [held]
    return pl.pallas_call(
        norm_bwd_kernel,
        grid=(far.shape[0] // tile,),
        in_specs=[whole, whole, row, part, piece, pl.BlockSpec((tile, 2 * HEAD_DIM), lambda i: (first + i, 0))] + [pl.BlockSpec(memory_space=pl.ANY)] * len(keep),
        out_specs=[whole, row],
        out_shape=[jax.ShapeDtypeStruct(x_seq.shape, jnp.bfloat16), jax.ShapeDtypeStruct((1, d_model), jnp.float32)],
        input_output_aliases={6: 0} if keep else {},
        scratch_shapes=[pltpu.VMEM((8, d_model), jnp.float32)],
        compiler_params=pltpu.CompilerParams(vmem_limit_bytes=62 * 2 ** 20),
        cost_estimate=pl.CostEstimate(flops=4 * 10 ** 9, bytes_accessed=16 * 10 ** 6, transcendentals=0),
        name="norm_bwd",
    )(x_seq, y_grad, gain, near, far, stat, *keep)


def proj_deep_kernel(n_parts, dims, *refs):
    parts, w_ref, outs, accs = refs[:n_parts], refs[n_parts], refs[n_parts + 1:2 * n_parts + 1], refs[2 * n_parts + 1:]
    step, last = pl.program_id(0), pl.num_programs(0) - 1

    @pl.when(step == 0)
    def _():
        for a, acc in zip(parts, accs):
            acc[...] = dot(a[...], w_ref[...], dims)

    @pl.when((step > 0) & (step < last))
    def _():
        for a, acc in zip(parts, accs):
            acc[...] += dot(a[...], w_ref[...], dims)

    @pl.when(step == last)
    def _():
        for a, acc, out in zip(parts, accs, outs):
            out[...] = (acc[...] + dot(a[...], w_ref[...], dims)).astype(jnp.bfloat16)


def part_spec(a, b, block, index):
    if a.ndim == 2:
        return pl.BlockSpec(block, index)
    return pl.BlockSpec((None,) + block, lambda i: (b,) + index(i))


def proj_deep(parts, w, dims, tile=1024):
    rows, depth = parts[0].shape[-2:]
    width = w.shape[0] if dims is NT else w.shape[1]
    w_spec = pl.BlockSpec((width, tile), lambda i: (0, i)) if dims is NT else pl.BlockSpec((tile, width), lambda i: (i, 0))
    return pl.pallas_call(
        functools.partial(proj_deep_kernel, len(parts), dims),
        grid=(depth // tile,),
        in_specs=[part_spec(a, b, (rows, tile), lambda i: (0, i)) for b, a in enumerate(parts)] + [w_spec],
        out_specs=[pl.BlockSpec((rows, width), lambda i: (0, 0))] * len(parts),
        out_shape=[jax.ShapeDtypeStruct((rows, width), jnp.bfloat16)] * len(parts),
        scratch_shapes=[pltpu.VMEM((rows, width), jnp.float32)] * len(parts),
        compiler_params=pltpu.CompilerParams(vmem_limit_bytes=62 * 2 ** 20),
        cost_estimate=pl.CostEstimate(flops=2 * len(parts) * rows * depth * width, bytes_accessed=2 * depth * width, transcendentals=0),
        name="proj_deep",
    )(*parts, w)


def proj_wide_kernel(n_parts, dims, *refs):
    w_ref = refs[n_parts]
    for a, out in zip(refs[:n_parts], refs[n_parts + 1:]):
        out[...] = dot(a[...], w_ref[...], dims).astype(jnp.bfloat16)


def proj_wide(parts, w, dims, tile=1024):
    rows, depth = parts[0].shape
    width = w.shape[0] if dims is NT else w.shape[1]
    w_spec = pl.BlockSpec((tile, depth), lambda i: (i, 0)) if dims is NT else pl.BlockSpec((depth, tile), lambda i: (0, i))
    return pl.pallas_call(
        functools.partial(proj_wide_kernel, len(parts), dims),
        grid=(width // tile,),
        in_specs=[pl.BlockSpec((rows, depth), lambda i: (0, 0))] * len(parts) + [w_spec],
        out_specs=[pl.BlockSpec((rows, tile), lambda i: (0, i))] * len(parts),
        out_shape=[jax.ShapeDtypeStruct((rows, width), jnp.bfloat16)] * len(parts),
        compiler_params=pltpu.CompilerParams(vmem_limit_bytes=62 * 2 ** 20),
        cost_estimate=pl.CostEstimate(flops=2 * len(parts) * rows * depth * width, bytes_accessed=2 * depth * width, transcendentals=0),
        name="proj_wide",
    )(*parts, w)


def solution(mesh):
    n_tp = mesh.shape["tp"]
    pairs = [[i, i + 1] for i in range(0, n_tp, 2)]

    def swap(value, bit):
        return lax.ppermute(value, "tp", [(i, i ^ bit) for i in range(n_tp)])

    def pair_gather(value, axis=0):
        return lax.all_gather(value, "tp", axis_index_groups=pairs, axis=axis, tiled=True)

    def pair_scatter(value):
        return lax.psum_scatter(value, "tp", axis_index_groups=pairs, scatter_dimension=0, tiled=True)

    def staged_step(x_seq, ln_gain, w_qkv, w_out, y_grad):
        kv_loc = w_qkv.shape[1]
        gain = ln_gain[None, :]
        token = [None]

        def run(fn, lead, *rest):
            if token[0] is not None:
                lead, _ = lax.optimization_barrier((lead, token[0]))
            result = fn(lead, *rest)
            token[0] = jax.tree.leaves(result)[0]
            return result

        cos_t, sin_t = rope_tables(x_seq.shape[1] * n_tp)
        h0, stat0 = run(lambda x: norm_fwd(x, gain, 0), x_seq)
        hx0 = swap(h0, 2)
        h1, stat1 = run(lambda x: norm_fwd(x, gain, 1), x_seq)
        hx1 = swap(h1, 2)
        dy0, dy1, _ = lax.optimization_barrier((y_grad[0], y_grad[1], h1))
        dyx0 = swap(dy0, 2)
        dyx1 = swap(dy1, 2)
        h_own0, h_own1 = pair_gather(h0), pair_gather(h1)
        dy_own = pair_gather(y_grad, 1)
        w_flat = run(lambda w: lax.optimization_barrier(w.reshape(w.shape[0], -1)), w_qkv)
        qkv_own0, qkv_own1 = run(lambda h: proj_deep([h, h_own1], w_flat, NN), h_own0)
        h_far0 = pair_gather(hx0)
        dattn_own0, dattn_own1 = run(lambda d: proj_deep([d, d], w_out, NT), dy_own)
        (qkv_far0,) = run(lambda h: proj_deep([h], w_flat, NN), h_far0)
        attn_own0, attn_far0, lse0 = run(lambda far: attn_fwd(qkv_own0, far, cos_t, sin_t, kv_loc), qkv_far0)
        h_far1 = pair_gather(hx1)
        o_far0, o_near0 = run(lambda a: proj_wide([a, attn_own0], w_out, NN), attn_far0)
        os_far0, os_near0 = pair_scatter(o_far0), pair_scatter(o_near0)
        (qkv_far1,) = run(lambda h: proj_deep([h], w_flat, NN), h_far1)
        ox0 = swap(os_far0, 2)
        attn_own1, attn_far1, lse1 = run(lambda far: attn_fwd(qkv_own1, far, cos_t, sin_t, kv_loc), qkv_far1)
        dy_far0 = pair_gather(dyx0)
        o_far1, o_near1 = run(lambda a: proj_wide([a, attn_own1], w_out, NN), attn_far1)
        os_far1, os_near1 = pair_scatter(o_far1), pair_scatter(o_near1)
        (dattn_far0,) = run(lambda d: proj_deep([d], w_out, NT), dy_far0)
        ox1 = swap(os_far1, 2)
        dq_own0, dq_far0 = run(lambda d: attn_bwd(qkv_own0, qkv_far0, attn_own0, attn_far0, dattn_own0, d, lse0, cos_t, sin_t, kv_loc), dattn_far0)
        dy_far1 = pair_gather(dyx1)
        dh_far0, dh_near0 = run(lambda d: proj_wide([d, dq_own0], w_flat, NT), dq_far0)
        dhs_far0, dhs_near0 = pair_scatter(dh_far0), pair_scatter(dh_near0)
        (dattn_far1,) = run(lambda d: proj_deep([d], w_out, NT), dy_far1)
        dhx0 = swap(dhs_far0, 2)
        dq_own1, dq_far1 = run(lambda d: attn_bwd(qkv_own1, qkv_far1, attn_own1, attn_far1, dattn_own1, d, lse1, cos_t, sin_t, kv_loc), dattn_far1)
        dh_far1, dh_near1 = run(lambda d: proj_wide([d, dq_own1], w_flat, NT), dq_far1)
        dhs_far1, dhs_near1 = pair_scatter(dh_far1), pair_scatter(dh_near1)
        wout_grad = run(lambda a: dw_out([a, attn_far0, attn_own1, attn_far1], [(0, dy_own), (0, dy_far0), (1, dy_own), (0, dy_far1)]), attn_own0)
        cut = dhs_far1.shape[0] // 2
        dhx1a, dhx1b = swap(dhs_far1[:cut], 2), swap(dhs_far1[cut:], 2)
        y_out = run(lambda near: residual(x_seq, [near, os_near1], [ox0, ox1]), os_near0)
        wqkv_grad = run(lambda h: dw_qkv([h, h_far0, h_own1, h_far1], [dq_own0, dq_far0, dq_own1, dq_far1], kv_loc), h_own0)
        x_grad, gain0 = run(lambda near: norm_bwd(x_seq, y_grad, gain, near, dhx0, stat0, 0, 0, None), dhs_near0)
        x_grad, gain1 = run(lambda near: norm_bwd(x_seq, y_grad, gain, near, dhx1a, stat1, 1, 0, x_grad), dhs_near1)
        x_grad, gain2 = run(lambda near: norm_bwd(x_seq, y_grad, gain, near, dhx1b, stat1, 1, cut, x_grad), dhs_near1)
        mine = gain0 + gain1 + gain2
        gain_grad = (mine + swap(mine, 1) + swap(mine, 2) + swap(mine, 3)).astype(jnp.bfloat16)[0]
        return y_out, x_grad, gain_grad, wqkv_grad, wout_grad

    specs_in = (P('dp', 'tp', None), P(None), P(None, 'tp', None), P('tp', None), P('dp', 'tp', None))
    specs_out = (P('dp', 'tp', None), P('dp', 'tp', None), P('dp'), P('dp', 'tp', None), P(('dp', 'tp'), None))
    return jax.shard_map(staged_step, mesh=mesh, in_specs=specs_in, out_specs=specs_out, check_vma=False)
```

```python
import functools
import jax
import jax.numpy as jnp
from jax import lax
from jax.experimental import pallas as pl
from jax.experimental.pallas import tpu as pltpu
from jax.sharding import PartitionSpec as P

CLIP_QKV = 8.0
ROPE_THETA = 500000.0
LN_EPS = 1e-5
LOG2E = 1.4426950408889634
HEAD_DIM = 128
TILE_Q = 256
NEG_BIG = -1e30
NT = (((1,), (1,)), ((), ()))
TN = (((0,), (0,)), ((), ()))
NN = (((1,), (0,)), ((), ()))


GRANT = pltpu.CompilerParams(vmem_limit_bytes=62 * 2 ** 20)


def cost(gigaflops, megabytes):
    return pl.CostEstimate(flops=gigaflops * 10 ** 9, bytes_accessed=megabytes * 10 ** 6, transcendentals=0)


def matmul_cost(rows, depth, width):
    return pl.CostEstimate(flops=2 * rows * depth * width, bytes_accessed=2 * depth * width, transcendentals=0)


def along_rows(rows, columns):
    return pl.BlockSpec((rows, columns), lambda i: (i, 0))


def along_columns(rows, columns):
    return pl.BlockSpec((rows, columns), lambda i: (0, i))


def held_whole(rows, columns):
    return pl.BlockSpec((rows, columns), lambda i: (0, 0))


def dot(a, b, dims):
    return lax.dot_general(a, b, dims, preferred_element_type=jnp.float32)


def rope_tables(positions):
    inv_freq = 1.0 / (ROPE_THETA ** (jnp.arange(0, HEAD_DIM, 2, dtype=jnp.float32) / HEAD_DIM))
    angles = positions[:, None] * inv_freq[None, :]
    cos_t, sin_t = jnp.cos(angles), jnp.sin(angles)
    return jnp.concatenate([cos_t, cos_t], axis=-1), jnp.concatenate([-sin_t, sin_t], axis=-1)


def clipped(raw):
    return jnp.minimum(jnp.maximum(raw.astype(jnp.float32), -CLIP_QKV), CLIP_QKV)


def rotate(vec, cos_t, sin_t):
    return (vec * cos_t + pltpu.roll(vec, HEAD_DIM // 2, 1) * sin_t).astype(jnp.bfloat16)


def unrotate(grad, cos_t, sin_t):
    grad = grad.astype(jnp.bfloat16).astype(jnp.float32)
    return grad * cos_t - pltpu.roll(grad, HEAD_DIM // 2, 1) * sin_t


def pass_clip(grad, raw):
    inside = jnp.abs(raw.astype(jnp.float32)) < CLIP_QKV
    return jnp.where(inside, grad, 0.0).astype(jnp.bfloat16)


def diagonal_mask():
    row = lax.broadcasted_iota(jnp.int32, (TILE_Q, TILE_Q), 0)
    col = lax.broadcasted_iota(jnp.int32, (TILE_Q, TILE_Q), 1)
    return row >= col


def half_rows(own, size):
    side = lax.axis_index("tp") // 2
    start = side if own else 1 - side
    return pl.ds(pl.multiple_of(start * size, size), size)


def attn_fwd_kernel(groups, own_ref, far_ref, cos_ref, sin_ref, oown_ref, ofar_ref, lse_ref, qkv_ref, out_ref, k_scr, v_scr, s_scr, p_scr):
    half = own_ref.shape[0]
    own, far = half_rows(True, half), half_rows(False, half)
    qkv_ref[own, :] = own_ref[...]
    qkv_ref[far, :] = far_ref[...]
    seq_len = qkv_ref.shape[0]
    k_col = groups * HEAD_DIM
    k_scr[...] = rotate(clipped(qkv_ref[:, k_col:k_col + HEAD_DIM]), cos_ref[...], sin_ref[...])
    v_scr[...] = clipped(qkv_ref[:, k_col + HEAD_DIM:k_col + 2 * HEAD_DIM]).T.astype(jnp.bfloat16)
    row = lax.broadcasted_iota(jnp.int32, (TILE_Q, TILE_Q), 0)
    col = lax.broadcasted_iota(jnp.int32, (TILE_Q, TILE_Q), 1)
    mask = row <= col
    coef = HEAD_DIM ** -0.5 * LOG2E

    def head(g, carry):
        cols = pl.ds(pl.multiple_of(g * HEAD_DIM, HEAD_DIM), HEAD_DIM)

        def scored(qi):
            rows = slice(qi * TILE_Q, (qi + 1) * TILE_Q)
            query = rotate(clipped(qkv_ref[rows, cols]), cos_ref[rows, :], sin_ref[rows, :])
            peak = None
            for kj in range(qi + 1):
                keys = slice(kj * TILE_Q, (kj + 1) * TILE_Q)
                scores = dot(k_scr[keys, :], query, NT)
                if kj == qi:
                    scores = jnp.where(mask, scores, NEG_BIG)
                s_scr[qi % 2, keys, :] = scores
                part = jnp.max(scores.reshape(TILE_Q // 8, 8, TILE_Q), axis=0)
                peak = part if peak is None else jnp.maximum(peak, part)
            return jnp.max(peak, axis=0, keepdims=True) * coef

        def mixed(qi, shift):
            rows = slice(qi * TILE_Q, (qi + 1) * TILE_Q)
            total = None
            for kj in range(qi + 1):
                keys = slice(kj * TILE_Q, (kj + 1) * TILE_Q)
                prob = jnp.exp2(s_scr[qi % 2, keys, :] * coef - shift)
                p_scr[qi % 2, keys, :] = prob.astype(jnp.bfloat16)
                part = jnp.sum(prob.reshape(TILE_Q // 8, 8, TILE_Q), axis=0)
                total = part if total is None else total + part
            total = jnp.sum(total, axis=0, keepdims=True)
            out = dot(v_scr[:, :(qi + 1) * TILE_Q], p_scr[qi % 2, :(qi + 1) * TILE_Q, :], NN)
            out_ref[rows, cols] = (out * (1.0 / total)).T.astype(jnp.bfloat16)
            lse_ref[rows, cols] = jnp.broadcast_to(shift + jnp.log2(total), (HEAD_DIM, TILE_Q)).T

        tiles = seq_len // TILE_Q
        shift = scored(0)
        for qi in range(tiles):
            later = scored(qi + 1) if qi + 1 < tiles else None
            mixed(qi, shift)
            shift = later
        return carry

    lax.fori_loop(0, groups, head, 0)
    oown_ref[...] = out_ref[own, :]
    ofar_ref[...] = out_ref[far, :]


def attn_bwd_kernel(groups, own_ref, far_ref, aown_ref, afar_ref, down_ref, dfar_ref, lse_ref, cos_ref, sin_ref, gown_ref, gfar_ref, qkv_ref, attn_ref, dattn_ref, k_scr, v_scr, dk_scr, dv_scr, q_scr, p_scr, s_scr):
    half = own_ref.shape[0]
    own, far = half_rows(True, half), half_rows(False, half)
    for dst, near, away in ((qkv_ref, own_ref, far_ref), (attn_ref, aown_ref, afar_ref), (dattn_ref, down_ref, dfar_ref)):
        dst[own, :] = near[...]
        dst[far, :] = away[...]
    seq_len = qkv_ref.shape[0]
    k_col = groups * HEAD_DIM
    v_col = k_col + HEAD_DIM
    scale = HEAD_DIM ** -0.5
    coef = scale * LOG2E
    k_scr[...] = rotate(clipped(qkv_ref[:, k_col:v_col]), cos_ref[...], sin_ref[...])
    v_scr[...] = clipped(qkv_ref[:, v_col:v_col + HEAD_DIM]).astype(jnp.bfloat16)
    dk_scr[...] = jnp.zeros_like(dk_scr)
    dv_scr[...] = jnp.zeros_like(dv_scr)
    mask = diagonal_mask()

    def head(g, carry):
        cols = pl.ds(pl.multiple_of(g * HEAD_DIM, HEAD_DIM), HEAD_DIM)

        def scored(qi):
            rows = slice(qi * TILE_Q, (qi + 1) * TILE_Q)
            query = rotate(clipped(qkv_ref[rows, cols]), cos_ref[rows, :], sin_ref[rows, :])
            q_scr[qi % 2] = query
            dout = dattn_ref[rows, cols]
            delta = jnp.sum(dout.astype(jnp.float32) * attn_ref[rows, cols].astype(jnp.float32), axis=1, keepdims=True)
            lse = jnp.concatenate([lse_ref[rows, cols]] * (TILE_Q // HEAD_DIM), axis=1)
            for kj in range(qi + 1):
                keys = slice(kj * TILE_Q, (kj + 1) * TILE_Q)
                scores = dot(query, k_scr[keys, :], NT)
                if kj == qi:
                    scores = jnp.where(mask, scores, NEG_BIG)
                prob = jnp.exp2(scores * coef - lse)
                dprob = dot(dout, v_scr[keys, :], NT).astype(jnp.bfloat16).astype(jnp.float32)
                p_scr[qi % 2, :, keys] = prob.astype(jnp.bfloat16)
                s_scr[qi % 2, :, keys] = (prob * (dprob - delta)).astype(jnp.bfloat16)

        def mixed(qi):
            rows = slice(qi * TILE_Q, (qi + 1) * TILE_Q)
            width = (qi + 1) * TILE_Q
            dscore = s_scr[qi % 2, :, :width]
            dv_scr[:, :width] += dot(dattn_ref[rows, cols], p_scr[qi % 2, :, :width], TN)
            dk_scr[:, :width] += dot(q_scr[qi % 2], dscore, TN)
            dquery = dot(dscore, k_scr[:width, :], NN) * scale
            qkv_ref[rows, cols] = pass_clip(unrotate(dquery, cos_ref[rows, :], sin_ref[rows, :]), qkv_ref[rows, cols])

        tiles = seq_len // TILE_Q
        scored(0)
        for qi in range(tiles):
            if qi + 1 < tiles:
                scored(qi + 1)
            mixed(qi)
        return carry

    lax.fori_loop(0, groups, head, 0)
    dkey = unrotate(dk_scr[...].T * scale, cos_ref[...], sin_ref[...])
    qkv_ref[:, k_col:v_col] = pass_clip(dkey, qkv_ref[:, k_col:v_col])
    qkv_ref[:, v_col:v_col + HEAD_DIM] = pass_clip(dv_scr[...].T, qkv_ref[:, v_col:v_col + HEAD_DIM])
    gown_ref[...] = qkv_ref[own, :]
    gfar_ref[...] = qkv_ref[far, :]


def head_specs(half, slot, wide):
    table = held_whole(2 * half, HEAD_DIM)
    part = along_columns(half, wide)
    full = along_columns(half, slot)
    lse = along_columns(2 * half, wide)
    return table, part, full, lse


def attn_fwd(qkv_own, qkv_far, cos_t, sin_t, kv_loc):
    half = qkv_own.shape[0]
    slot = qkv_own.shape[1] // kv_loc
    groups = slot // HEAD_DIM - 2
    wide = groups * HEAD_DIM
    table, part, full, lse = head_specs(half, slot, wide)
    rows = jax.ShapeDtypeStruct((half, kv_loc * wide), jnp.bfloat16)
    return pl.pallas_call(
        functools.partial(attn_fwd_kernel, groups),
        grid=(kv_loc,),
        in_specs=[full, full, table, table],
        out_specs=[part, part, lse],
        out_shape=[rows, rows, jax.ShapeDtypeStruct((2 * half, kv_loc * wide), jnp.float32)],
        scratch_shapes=[pltpu.VMEM((2 * half, slot), jnp.bfloat16), pltpu.VMEM((2 * half, wide), jnp.bfloat16), pltpu.VMEM((2 * half, HEAD_DIM), jnp.bfloat16), pltpu.VMEM((HEAD_DIM, 2 * half), jnp.bfloat16), pltpu.VMEM((2, 2 * half, TILE_Q), jnp.float32), pltpu.VMEM((2, 2 * half, TILE_Q), jnp.bfloat16)],
        compiler_params=GRANT,
        cost_estimate=cost(12, 14),
        name="attn_fwd",
    )(qkv_own, qkv_far, cos_t, sin_t)


def attn_bwd(qkv_own, qkv_far, attn_own, attn_far, dattn_own, dattn_far, lse_t, cos_t, sin_t, kv_loc):
    half = qkv_own.shape[0]
    slot = qkv_own.shape[1] // kv_loc
    groups = slot // HEAD_DIM - 2
    wide = groups * HEAD_DIM
    table, part, full, lse = head_specs(half, slot, wide)
    return pl.pallas_call(
        functools.partial(attn_bwd_kernel, groups),
        grid=(kv_loc,),
        in_specs=[full, full, part, part, part, part, lse, table, table],
        out_specs=[full, full],
        out_shape=[jax.ShapeDtypeStruct(qkv_own.shape, jnp.bfloat16)] * 2,
        scratch_shapes=[pltpu.VMEM((2 * half, slot), jnp.bfloat16)] + [pltpu.VMEM((2 * half, wide), jnp.bfloat16)] * 2 + [pltpu.VMEM((2 * half, HEAD_DIM), jnp.bfloat16)] * 2 + [pltpu.VMEM((HEAD_DIM, 2 * half), jnp.float32)] * 2 + [pltpu.VMEM((2, TILE_Q, HEAD_DIM), jnp.bfloat16)] + [pltpu.VMEM((2, TILE_Q, 2 * half), jnp.bfloat16)] * 2,
        compiler_params=GRANT,
        cost_estimate=cost(25, 22),
        name="attn_bwd",
    )(qkv_own, qkv_far, attn_own, attn_far, dattn_own, dattn_far, lse_t, cos_t, sin_t)


def dw_qkv_kernel(n_rows, *refs):
    acts, grads, out_ref = refs[:n_rows], refs[n_rows:-1], refs[-1]
    slot = out_ref.shape[2]
    for n in range(out_ref.shape[1]):
        cols = slice(n * slot, (n + 1) * slot)
        acc = sum(dot(a[...], g[:, cols], TN) for a, g in zip(acts, grads))
        out_ref[:, n, :] = acc.astype(jnp.bfloat16)


def dw_qkv(acts, grads, kv_loc, tile=512):
    rows, d_model = acts[0].shape
    width = grads[0].shape[1]
    slot = width // kv_loc
    whole = held_whole(rows, width)
    part = along_columns(rows, tile)
    return pl.pallas_call(
        functools.partial(dw_qkv_kernel, len(acts)),
        grid=(d_model // tile,),
        in_specs=[part] * len(acts) + [whole] * len(grads),
        out_specs=pl.BlockSpec((tile, kv_loc, slot), lambda i: (i, 0, 0)),
        out_shape=jax.ShapeDtypeStruct((d_model, kv_loc, slot), jnp.bfloat16),
        compiler_params=GRANT,
        cost_estimate=cost(51, 60),
        name="dw_qkv",
    )(*acts, *grads)


def dw_out_kernel(n_rows, *refs):
    acts, grads, out_ref = refs[:n_rows], refs[n_rows:-1], refs[-1]
    out_ref[...] = sum(dot(a[...], g[...], TN) for a, g in zip(acts, grads)).astype(jnp.bfloat16)


def dw_out(acts, grads, tile=512):
    rows, width = acts[0].shape
    d_model = grads[0][1].shape[-1]
    whole = held_whole(rows, width)
    return pl.pallas_call(
        functools.partial(dw_out_kernel, len(acts)),
        grid=(d_model // tile,),
        in_specs=[whole] * len(acts) + [part_spec(g, b, (rows, tile), lambda i: (0, i)) for b, g in grads],
        out_specs=along_columns(width, tile),
        out_shape=jax.ShapeDtypeStruct((width, d_model), jnp.bfloat16),
        compiler_params=GRANT,
        cost_estimate=cost(39, 50),
        name="dw_out",
    )(*acts, *[g for _, g in grads])


def norm_fwd_kernel(x_ref, gain_ref, h_ref, stat_ref):
    def group(i, carry):
        rows = pl.ds(pl.multiple_of(i * 16, 16), 16)
        x_f32 = x_ref[0, rows, :].astype(jnp.float32)
        mean = jnp.mean(x_f32, axis=-1, keepdims=True)
        centered = x_f32 - mean
        rstd = lax.rsqrt(jnp.mean(centered * centered, axis=-1, keepdims=True) + LN_EPS)
        h_ref[rows, :] = (centered * rstd * gain_ref[...].astype(jnp.float32)).astype(jnp.bfloat16)
        stat_ref[rows, :HEAD_DIM] = jnp.broadcast_to(mean, (16, HEAD_DIM))
        stat_ref[rows, HEAD_DIM:] = jnp.broadcast_to(rstd, (16, HEAD_DIM))
        return carry

    lax.fori_loop(0, x_ref.shape[1] // 16, group, 0, unroll=True)


def norm_fwd(x_seq, gain, b, tile=64):
    _, rows, d_model = x_seq.shape
    return pl.pallas_call(
        norm_fwd_kernel,
        grid=(rows // tile,),
        in_specs=[pl.BlockSpec((1, tile, d_model), lambda i: (b, i, 0)), held_whole(1, d_model)],
        out_specs=[along_rows(tile, d_model), along_rows(tile, 2 * HEAD_DIM)],
        out_shape=[jax.ShapeDtypeStruct((rows, d_model), jnp.bfloat16), jax.ShapeDtypeStruct((rows, 2 * HEAD_DIM), jnp.float32)],
        compiler_params=GRANT,
        cost_estimate=cost(2, 7),
        name="norm_fwd",
    )(x_seq, gain)


def norm_split_kernel(x_ref, gain_ref, dy_ref, h_ref, stat_ref, dy0_ref, dy1_ref):
    norm_fwd_kernel(x_ref, gain_ref, h_ref, stat_ref)
    dy0_ref[...] = dy_ref[0]
    dy1_ref[...] = dy_ref[1]


def norm_split(x_seq, gain, y_grad, b, lead=64):
    _, rows, d_model = x_seq.shape
    row = along_rows(lead, d_model)
    return pl.pallas_call(
        norm_split_kernel,
        grid=(rows // lead,),
        in_specs=[pl.BlockSpec((1, lead, d_model), lambda i: (b, i, 0)), held_whole(1, d_model), pl.BlockSpec((2, lead, d_model), lambda i: (0, i, 0))],
        out_specs=[row, along_rows(lead, 2 * HEAD_DIM), row, row],
        out_shape=[jax.ShapeDtypeStruct((rows, d_model), jnp.bfloat16), jax.ShapeDtypeStruct((rows, 2 * HEAD_DIM), jnp.float32), jax.ShapeDtypeStruct((rows, d_model), jnp.bfloat16), jax.ShapeDtypeStruct((rows, d_model), jnp.bfloat16)],
        compiler_params=GRANT,
        cost_estimate=cost(2, 19),
        name="norm_split",
    )(x_seq, gain, y_grad)


def residual_kernel(split, x_ref, near0_ref, near1_ref, far0_ref, far1_ref, out_ref):
    def add(near, far):
        out_ref[0] = (x_ref[0].astype(jnp.float32) + (near[...] + far[...]).astype(jnp.float32)).astype(jnp.bfloat16)

    pl.when(pl.program_id(0) < split)(lambda: add(near0_ref, far0_ref))
    pl.when(pl.program_id(0) >= split)(lambda: add(near1_ref, far1_ref))


def residual_last_kernel(x_ref, near_ref, far_ref, held_ref, out_ref):
    out_ref[0] = (x_ref[0].astype(jnp.float32) + (near_ref[...] + far_ref[...]).astype(jnp.float32)).astype(jnp.bfloat16)


def norm_bwd_kernel(x_ref, dy_ref, gain_ref, near_ref, far_ref, stat_ref, *rest):
    dx_ref, dgain_ref, sum_ref = rest[-3:]

    @pl.when(pl.program_id(0) == 0)
    def _():
        sum_ref[...] = jnp.zeros_like(sum_ref)

    def group(i, carry):
        rows = pl.ds(pl.multiple_of(i * 16, 16), 16)
        mean, rstd = stat_ref[rows, :1], stat_ref[rows, HEAD_DIM:HEAD_DIM + 1]
        hat = (x_ref[0, rows, :].astype(jnp.float32) - mean) * rstd
        dh = (near_ref[rows, :] + far_ref[rows, :]).astype(jnp.float32)
        prod = dh * hat
        sum_ref[...] += prod[:8] + prod[8:]
        dhat = dh * gain_ref[...].astype(jnp.float32)
        inner = dhat - jnp.mean(dhat, axis=-1, keepdims=True) - hat * jnp.mean(dhat * hat, axis=-1, keepdims=True)
        dx_ref[0, rows, :] = (dy_ref[0, rows, :].astype(jnp.float32) + inner * rstd).astype(jnp.bfloat16)
        return carry

    lax.fori_loop(0, x_ref.shape[1] // 16, group, 0, unroll=2)

    @pl.when(pl.program_id(0) == pl.num_programs(0) - 1)
    def _():
        dgain_ref[...] = jnp.sum(sum_ref[...], axis=0, keepdims=True)


def residual(x_seq, nears, fars, tile=64):
    _, rows, d_model = x_seq.shape
    split = rows // tile
    whole = pl.BlockSpec((1, tile, d_model), lambda i: (i // split, lax.rem(i, split), 0))
    first = pl.BlockSpec((tile, d_model), lambda i: (jnp.minimum(i, split - 1), 0))
    second = pl.BlockSpec((tile, d_model), lambda i: (jnp.maximum(i - split, 0), 0))
    return pl.pallas_call(
        functools.partial(residual_kernel, split),
        grid=(split + fars[1].shape[0] // tile,),
        in_specs=[whole, first, second, first, second],
        out_specs=whole,
        out_shape=jax.ShapeDtypeStruct(x_seq.shape, jnp.bfloat16),
        compiler_params=GRANT,
        cost_estimate=cost(4, 26),
        name="residual",
    )(x_seq, *nears, *fars)


def residual_last(x_seq, near, far, held, tile=32):
    _, rows, d_model = x_seq.shape
    base = (rows - far.shape[0]) // tile
    whole = pl.BlockSpec((1, tile, d_model), lambda i: (1, base + i, 0))
    return pl.pallas_call(
        residual_last_kernel,
        grid=(far.shape[0] // tile,),
        in_specs=[whole, pl.BlockSpec((tile, d_model), lambda i: (base + i, 0)), along_rows(tile, d_model), pl.BlockSpec(memory_space=pl.ANY)],
        out_specs=whole,
        out_shape=jax.ShapeDtypeStruct(x_seq.shape, jnp.bfloat16),
        input_output_aliases={3: 0},
        compiler_params=GRANT,
        cost_estimate=cost(1, 3),
        name="residual_last",
    )(x_seq, near, far, held)


def norm_bwd(x_seq, y_grad, gain, near, far, stat, b, base, held, tile=64):
    _, _, d_model = x_seq.shape
    first = base // tile
    whole = pl.BlockSpec((1, tile, d_model), lambda i: (b, first + i, 0))
    part = pl.BlockSpec((tile, d_model), lambda i: (first + i, 0))
    piece = along_rows(tile, d_model)
    row = held_whole(1, d_model)
    keep = [] if held is None else [held]
    return pl.pallas_call(
        norm_bwd_kernel,
        grid=(far.shape[0] // tile,),
        in_specs=[whole, whole, row, part, piece, pl.BlockSpec((tile, 2 * HEAD_DIM), lambda i: (first + i, 0))] + [pl.BlockSpec(memory_space=pl.ANY)] * len(keep),
        out_specs=[whole, row],
        out_shape=[jax.ShapeDtypeStruct(x_seq.shape, jnp.bfloat16), jax.ShapeDtypeStruct((1, d_model), jnp.float32)],
        input_output_aliases={6: 0} if keep else {},
        scratch_shapes=[pltpu.VMEM((8, d_model), jnp.float32)],
        compiler_params=GRANT,
        cost_estimate=cost(4, 16),
        name="norm_bwd",
    )(x_seq, y_grad, gain, near, far, stat, *keep)


def proj_deep_kernel(dims, a_ref, w_ref, out_ref, acc_ref):
    step, last = pl.program_id(0), pl.num_programs(0) - 1

    @pl.when(step == 0)
    def _():
        acc_ref[...] = jnp.zeros_like(acc_ref)

    acc_ref[...] += dot(a_ref[...], w_ref[...], dims)

    @pl.when(step == last)
    def _():
        out_ref[...] = acc_ref[...].astype(jnp.bfloat16)


def part_spec(a, b, block, index):
    if a.ndim == 2:
        return pl.BlockSpec(block, index)
    return pl.BlockSpec((None,) + block, lambda i: (b,) + index(i))


def proj_raw_kernel(n_parts, *refs):
    mine, theirs, w_ref = refs[:n_parts], refs[n_parts:2 * n_parts], refs[2 * n_parts]
    outs, flat_ref = refs[2 * n_parts + 1:3 * n_parts + 1], refs[3 * n_parts + 1]
    accs, joined = refs[3 * n_parts + 2:-1], refs[-1]
    step, last = pl.program_id(0), pl.num_programs(0) - 1
    core = lax.rem(lax.axis_index("tp"), 2)
    rows = mine[0].shape[0]

    @pl.when(step == 0)
    def _():
        for acc in accs:
            acc[...] = jnp.zeros_like(acc)

    flat_ref[...] = w_ref[...].reshape(flat_ref.shape)
    for b in range(n_parts):
        joined[b, pl.ds(pl.multiple_of(core * rows, rows), rows), :] = mine[b][...]
        joined[b, pl.ds(pl.multiple_of((1 - core) * rows, rows), rows), :] = theirs[b][...]
    for b, acc in enumerate(accs):
        acc[...] += dot(joined[b], flat_ref[...], NN)

    @pl.when(step == last)
    def _():
        for acc, out in zip(accs, outs):
            out[...] = acc[...].astype(jnp.bfloat16)


def proj_raw(mine, theirs, w, tile=512):
    rows, depth = mine[0].shape
    n_parts = len(mine)
    slots, slot = w.shape[1:]
    width = slots * slot
    return pl.pallas_call(
        functools.partial(proj_raw_kernel, n_parts),
        grid=(depth // tile,),
        in_specs=[along_columns(rows, tile)] * (2 * n_parts) + [pl.BlockSpec((tile, slots, slot), lambda i: (i, 0, 0))],
        out_specs=[held_whole(2 * rows, width)] * n_parts + [along_rows(tile, width)],
        out_shape=[jax.ShapeDtypeStruct((2 * rows, width), jnp.bfloat16)] * n_parts + [jax.ShapeDtypeStruct((depth, width), jnp.bfloat16)],
        scratch_shapes=[pltpu.VMEM((2 * rows, width), jnp.float32)] * n_parts + [pltpu.VMEM((n_parts, 2 * rows, tile), jnp.bfloat16)],
        compiler_params=GRANT,
        cost_estimate=matmul_cost(2 * n_parts * rows, depth, width),
        name="proj_raw",
    )(*mine, *theirs, w)


def proj_deep(a, w, dims, b=0, tile=1024):
    rows, depth = a.shape[-2:]
    width = w.shape[0] if dims is NT else w.shape[1]
    return pl.pallas_call(
        functools.partial(proj_deep_kernel, dims),
        grid=(depth // tile,),
        in_specs=[part_spec(a, b, (rows, tile), lambda i: (0, i)), along_columns(width, tile) if dims is NT else along_rows(tile, width)],
        out_specs=held_whole(rows, width),
        out_shape=jax.ShapeDtypeStruct((rows, width), jnp.bfloat16),
        scratch_shapes=[pltpu.VMEM((rows, width), jnp.float32)],
        compiler_params=GRANT,
        cost_estimate=matmul_cost(rows, depth, width),
        name="proj_deep",
    )(a, w)


def proj_wide_kernel(n_parts, dims, cut, *refs):
    w_ref, outs = refs[n_parts], refs[n_parts + 1:]
    first = dot(refs[0][...], w_ref[...], dims).astype(jnp.bfloat16)
    half, rest = first.shape[0] // 2, outs[1:]
    if cut == half:
        outs[0][...] = first
    else:
        rest = outs[2:]
        outs[0][:cut], outs[0][cut:] = first[:cut], first[half:half + cut]
        outs[1][:half - cut], outs[1][half - cut:] = first[cut:half], first[half + cut:]
    for a, out in zip(refs[1:n_parts], rest):
        out[...] = dot(a[...], w_ref[...], dims).astype(jnp.bfloat16)


def proj_wide(parts, w, dims, cut=None, tile=1024):
    rows, depth = parts[0].shape
    cut = cut or rows // 2
    width = w.shape[0] if dims is NT else w.shape[1]
    w_spec = along_rows(tile, depth) if dims is NT else along_columns(depth, tile)
    sizes = [2 * cut] + [rows - 2 * cut] * (2 * cut < rows) + [rows] * (len(parts) - 1)
    return pl.pallas_call(
        functools.partial(proj_wide_kernel, len(parts), dims, cut),
        grid=(width // tile,),
        in_specs=[held_whole(rows, depth)] * len(parts) + [w_spec],
        out_specs=[along_columns(size, tile) for size in sizes],
        out_shape=[jax.ShapeDtypeStruct((size, width), jnp.bfloat16) for size in sizes],
        compiler_params=GRANT,
        cost_estimate=matmul_cost(len(parts) * rows, depth, width),
        name="proj_wide",
    )(*parts, w)


def solution(mesh):
    n_tp = mesh.shape["tp"]
    pairs = [[i, i + 1] for i in range(0, n_tp, 2)]

    def swap(value, bit):
        return lax.ppermute(value, "tp", [(i, i ^ bit) for i in range(n_tp)])

    def pair_gather(value, axis=0):
        return lax.all_gather(value, "tp", axis_index_groups=pairs, axis=axis, tiled=True)

    def pair_scatter(value):
        return lax.psum_scatter(value, "tp", axis_index_groups=pairs, scatter_dimension=0, tiled=True)

    def staged_step(x_seq, ln_gain, w_qkv, w_out, y_grad):
        kv_loc = w_qkv.shape[1]
        gain = ln_gain[None, :]
        token = [None]

        def run(fn, lead, *rest):
            if token[0] is not None:
                lead, _ = lax.optimization_barrier((lead, token[0]))
            result = fn(lead, *rest)
            token[0] = jax.tree.leaves(result)[0]
            return result

        h0, stat0 = run(lambda x: norm_fwd(x, gain, 0), x_seq)
        hx0 = swap(h0, 2)
        hs0 = swap(h0, 1)
        h1, stat1, dy0, dy1 = run(lambda x: norm_split(x, gain, y_grad, 1), x_seq)
        hs1 = swap(h1, 1)
        hx1 = swap(h1, 2)
        dyx0 = swap(dy0, 2)
        dyx1 = swap(dy1, 2)
        h_own0, h_own1 = pair_gather(h0), pair_gather(h1)
        dy_own = pair_gather(y_grad, 1)
        cos_t, sin_t = run(lambda p: lax.optimization_barrier(rope_tables(p)), jnp.arange(x_seq.shape[1] * n_tp, dtype=jnp.float32))
        qkv_own0, qkv_own1, w_flat = run(lambda h: proj_raw([h, h1], [hs0, hs1], w_qkv), h0)
        dattn_own0 = run(lambda d: proj_deep(d, w_out, NT, 0), dy_own)
        h_far0 = pair_gather(hx0)
        dattn_own1 = run(lambda d: proj_deep(d, w_out, NT, 1), dy_own)
        qkv_far0 = run(lambda h: proj_deep(h, w_flat, NN), h_far0)
        attn_own0, attn_far0, lse0 = run(lambda far: attn_fwd(qkv_own0, far, cos_t, sin_t, kv_loc), qkv_far0)
        h_far1 = pair_gather(hx1)
        o_far0, o_near0 = run(lambda a: proj_wide([a, attn_own0], w_out, NN), attn_far0)
        os_far0, os_near0 = pair_scatter(o_far0), pair_scatter(o_near0)
        qkv_far1 = run(lambda h: proj_deep(h, w_flat, NN), h_far1)
        ox0 = swap(os_far0, 2)
        attn_own1, attn_far1, lse1 = run(lambda far: attn_fwd(qkv_own1, far, cos_t, sin_t, kv_loc), qkv_far1)
        dy_far0 = pair_gather(dyx0)
        cut = x_seq.shape[1] * 3 // 4
        o_far1a, o_far1b, o_near1 = run(lambda a: proj_wide([a, attn_own1], w_out, NN, cut), attn_far1)
        os_far1a, os_far1b = pair_scatter(o_far1a), pair_scatter(o_far1b)
        os_near1 = pair_scatter(o_near1)
        dattn_far0 = run(lambda d: proj_deep(d, w_out, NT), dy_far0)
        ox1a, ox1b = swap(os_far1a, 2), swap(os_far1b, 2)
        dq_own0, dq_far0 = run(lambda d: attn_bwd(qkv_own0, qkv_far0, attn_own0, attn_far0, dattn_own0, d, lse0, cos_t, sin_t, kv_loc), dattn_far0)
        dy_far1 = pair_gather(dyx1)
        dh_far0, dh_near0 = run(lambda d: proj_wide([d, dq_own0], w_flat, NT), dq_far0)
        dhs_far0, dhs_near0 = pair_scatter(dh_far0), pair_scatter(dh_near0)
        dattn_far1 = run(lambda d: proj_deep(d, w_out, NT), dy_far1)
        dhx0 = swap(dhs_far0, 2)
        dq_own1, dq_far1 = run(lambda d: attn_bwd(qkv_own1, qkv_far1, attn_own1, attn_far1, dattn_own1, d, lse1, cos_t, sin_t, kv_loc), dattn_far1)
        dh_far1, dh_near1 = run(lambda d: proj_wide([d, dq_own1], w_flat, NT), dq_far1)
        dhs_far1, dhs_near1 = pair_scatter(dh_far1), pair_scatter(dh_near1)
        wout_grad = run(lambda a: dw_out([a, attn_far0, attn_own1, attn_far1], [(0, dy_own), (0, dy_far0), (1, dy_own), (0, dy_far1)]), attn_own0)
        dhx1 = swap(dhs_far1, 2)
        y_out = run(lambda near: residual(x_seq, [near, os_near1], [ox0, ox1a]), os_near0)
        wqkv_grad = run(lambda h: dw_qkv([h, h_far0, h_own1, h_far1], [dq_own0, dq_far0, dq_own1, dq_far1], kv_loc), h_own0)
        x_grad, gain0 = run(lambda near: norm_bwd(x_seq, y_grad, gain, near, dhx0, stat0, 0, 0, None), dhs_near0)
        x_grad, gain1 = run(lambda near: norm_bwd(x_seq, y_grad, gain, near, dhx1, stat1, 1, 0, x_grad), dhs_near1)
        y_out = run(lambda near: residual_last(x_seq, near, ox1b, y_out), os_near1)
        mine = gain0 + gain1
        gain_grad = (mine + swap(mine, 1) + swap(mine, 2) + swap(mine, 3)).astype(jnp.bfloat16)[0]
        return y_out, x_grad, gain_grad, wqkv_grad, wout_grad

    specs_in = (P('dp', 'tp', None), P(None), P(None, 'tp', None), P('tp', None), P('dp', 'tp', None))
    specs_out = (P('dp', 'tp', None), P('dp', 'tp', None), P('dp'), P('dp', 'tp', None), P(('dp', 'tp'), None))
    return jax.shard_map(staged_step, mesh=mesh, in_specs=specs_in, out_specs=specs_out, check_vma=False)
```

```python
import functools
import jax
import jax.numpy as jnp
from jax import lax
from jax.experimental import pallas as pl
from jax.experimental.pallas import tpu as pltpu
from jax.sharding import PartitionSpec as P

CLIP_QKV = 8.0
ROPE_THETA = 500000.0
LN_EPS = 1e-5
LOG2E = 1.4426950408889634
HEAD_DIM = 128
TILE_Q = 256
NEG_BIG = -1e30
NT = (((1,), (1,)), ((), ()))
TN = (((0,), (0,)), ((), ()))
NN = (((1,), (0,)), ((), ()))


GRANT = pltpu.CompilerParams(vmem_limit_bytes=62 * 2 ** 20)


def cost(gigaflops, megabytes):
    return pl.CostEstimate(flops=gigaflops * 10 ** 9, bytes_accessed=megabytes * 10 ** 6, transcendentals=0)


def matmul_cost(rows, depth, width):
    return pl.CostEstimate(flops=2 * rows * depth * width, bytes_accessed=2 * depth * width, transcendentals=0)


def along_rows(rows, columns):
    return pl.BlockSpec((rows, columns), lambda i: (i, 0))


def along_columns(rows, columns):
    return pl.BlockSpec((rows, columns), lambda i: (0, i))


def held_whole(rows, columns):
    return pl.BlockSpec((rows, columns), lambda i: (0, 0))


def dot(a, b, dims):
    return lax.dot_general(a, b, dims, preferred_element_type=jnp.float32)


def rope_tables(positions):
    inv_freq = 1.0 / (ROPE_THETA ** (jnp.arange(0, HEAD_DIM, 2, dtype=jnp.float32) / HEAD_DIM))
    angles = positions[:, None] * inv_freq[None, :]
    cos_t, sin_t = jnp.cos(angles), jnp.sin(angles)
    return jnp.concatenate([cos_t, cos_t], axis=-1), jnp.concatenate([-sin_t, sin_t], axis=-1)


def clipped(raw):
    return jnp.minimum(jnp.maximum(raw.astype(jnp.float32), -CLIP_QKV), CLIP_QKV)


def rotate(vec, cos_t, sin_t):
    return (vec * cos_t + pltpu.roll(vec, HEAD_DIM // 2, 1) * sin_t).astype(jnp.bfloat16)


def unrotate(grad, cos_t, sin_t):
    grad = grad.astype(jnp.bfloat16).astype(jnp.float32)
    return grad * cos_t - pltpu.roll(grad, HEAD_DIM // 2, 1) * sin_t


def pass_clip(grad, raw):
    inside = jnp.abs(raw.astype(jnp.float32)) < CLIP_QKV
    return jnp.where(inside, grad, 0.0).astype(jnp.bfloat16)


def diagonal_mask():
    row = lax.broadcasted_iota(jnp.int32, (TILE_Q, TILE_Q), 0)
    col = lax.broadcasted_iota(jnp.int32, (TILE_Q, TILE_Q), 1)
    return row >= col


def half_rows(own, size):
    side = lax.axis_index("tp") // 2
    start = side if own else 1 - side
    return pl.ds(pl.multiple_of(start * size, size), size)


def attn_fwd_kernel(groups, own_ref, far_ref, cos_ref, sin_ref, oown_ref, ofar_ref, lse_ref, qkv_ref, out_ref, k_scr, v_scr, s_scr, p_scr):
    half = own_ref.shape[0]
    own, far = half_rows(True, half), half_rows(False, half)
    qkv_ref[own, :] = own_ref[...]
    qkv_ref[far, :] = far_ref[...]
    seq_len = qkv_ref.shape[0]
    k_col = groups * HEAD_DIM
    k_scr[...] = rotate(clipped(qkv_ref[:, k_col:k_col + HEAD_DIM]), cos_ref[...], sin_ref[...])
    v_scr[...] = clipped(qkv_ref[:, k_col + HEAD_DIM:k_col + 2 * HEAD_DIM]).T.astype(jnp.bfloat16)
    row = lax.broadcasted_iota(jnp.int32, (TILE_Q, TILE_Q), 0)
    col = lax.broadcasted_iota(jnp.int32, (TILE_Q, TILE_Q), 1)
    mask = row <= col
    coef = HEAD_DIM ** -0.5 * LOG2E

    def head(g, carry):
        cols = pl.ds(pl.multiple_of(g * HEAD_DIM, HEAD_DIM), HEAD_DIM)

        def scored(qi):
            rows = slice(qi * TILE_Q, (qi + 1) * TILE_Q)
            query = rotate(clipped(qkv_ref[rows, cols]), cos_ref[rows, :], sin_ref[rows, :])
            peak = None
            for kj in range(qi + 1):
                keys = slice(kj * TILE_Q, (kj + 1) * TILE_Q)
                scores = dot(k_scr[keys, :], query, NT)
                if kj == qi:
                    scores = jnp.where(mask, scores, NEG_BIG)
                s_scr[qi % 2, keys, :] = scores
                part = jnp.max(scores.reshape(TILE_Q // 8, 8, TILE_Q), axis=0)
                peak = part if peak is None else jnp.maximum(peak, part)
            return jnp.max(peak, axis=0, keepdims=True) * coef

        def mixed(qi, shift):
            rows = slice(qi * TILE_Q, (qi + 1) * TILE_Q)
            total = None
            for kj in range(qi + 1):
                keys = slice(kj * TILE_Q, (kj + 1) * TILE_Q)
                prob = jnp.exp2(s_scr[qi % 2, keys, :] * coef - shift)
                p_scr[qi % 2, keys, :] = prob.astype(jnp.bfloat16)
                part = jnp.sum(prob.reshape(TILE_Q // 8, 8, TILE_Q), axis=0)
                total = part if total is None else total + part
            total = jnp.sum(total, axis=0, keepdims=True)
            out = dot(v_scr[:, :(qi + 1) * TILE_Q], p_scr[qi % 2, :(qi + 1) * TILE_Q, :], NN)
            out_ref[rows, cols] = (out * (1.0 / total)).T.astype(jnp.bfloat16)
            lse_ref[rows, cols] = jnp.broadcast_to(shift + jnp.log2(total), (HEAD_DIM, TILE_Q)).T

        tiles = seq_len // TILE_Q
        shift = scored(0)
        for qi in range(tiles):
            later = scored(qi + 1) if qi + 1 < tiles else None
            mixed(qi, shift)
            shift = later
        return carry

    lax.fori_loop(0, groups, head, 0)
    oown_ref[...] = out_ref[own, :]
    ofar_ref[...] = out_ref[far, :]


def attn_bwd_kernel(groups, own_ref, far_ref, aown_ref, afar_ref, down_ref, dfar_ref, lse_ref, cos_ref, sin_ref, gown_ref, gfar_ref, qkv_ref, attn_ref, dattn_ref, k_scr, v_scr, dk_scr, dv_scr, q_scr, p_scr, s_scr):
    half = own_ref.shape[0]
    own, far = half_rows(True, half), half_rows(False, half)
    for dst, near, away in ((qkv_ref, own_ref, far_ref), (attn_ref, aown_ref, afar_ref), (dattn_ref, down_ref, dfar_ref)):
        dst[own, :] = near[...]
        dst[far, :] = away[...]
    seq_len = qkv_ref.shape[0]
    k_col = groups * HEAD_DIM
    v_col = k_col + HEAD_DIM
    scale = HEAD_DIM ** -0.5
    coef = scale * LOG2E
    k_scr[...] = rotate(clipped(qkv_ref[:, k_col:v_col]), cos_ref[...], sin_ref[...])
    v_scr[...] = clipped(qkv_ref[:, v_col:v_col + HEAD_DIM]).astype(jnp.bfloat16)
    dk_scr[...] = jnp.zeros_like(dk_scr)
    dv_scr[...] = jnp.zeros_like(dv_scr)
    mask = diagonal_mask()

    def head(g, carry):
        cols = pl.ds(pl.multiple_of(g * HEAD_DIM, HEAD_DIM), HEAD_DIM)

        def scored(qi):
            rows = slice(qi * TILE_Q, (qi + 1) * TILE_Q)
            query = rotate(clipped(qkv_ref[rows, cols]), cos_ref[rows, :], sin_ref[rows, :])
            q_scr[qi % 2] = query
            dout = dattn_ref[rows, cols]
            delta = jnp.sum(dout.astype(jnp.float32) * attn_ref[rows, cols].astype(jnp.float32), axis=1, keepdims=True)
            lse = jnp.concatenate([lse_ref[rows, cols]] * (TILE_Q // HEAD_DIM), axis=1)
            for kj in range(qi + 1):
                keys = slice(kj * TILE_Q, (kj + 1) * TILE_Q)
                scores = dot(query, k_scr[keys, :], NT)
                if kj == qi:
                    scores = jnp.where(mask, scores, NEG_BIG)
                prob = jnp.exp2(scores * coef - lse)
                dprob = dot(dout, v_scr[keys, :], NT).astype(jnp.bfloat16).astype(jnp.float32)
                p_scr[qi % 2, :, keys] = prob.astype(jnp.bfloat16)
                s_scr[qi % 2, :, keys] = (prob * (dprob - delta)).astype(jnp.bfloat16)

        def mixed(qi):
            rows = slice(qi * TILE_Q, (qi + 1) * TILE_Q)
            width = (qi + 1) * TILE_Q
            dscore = s_scr[qi % 2, :, :width]
            dv_scr[:, :width] += dot(dattn_ref[rows, cols], p_scr[qi % 2, :, :width], TN)
            dk_scr[:, :width] += dot(q_scr[qi % 2], dscore, TN)
            dquery = dot(dscore, k_scr[:width, :], NN) * scale
            qkv_ref[rows, cols] = pass_clip(unrotate(dquery, cos_ref[rows, :], sin_ref[rows, :]), qkv_ref[rows, cols])

        tiles = seq_len // TILE_Q
        scored(0)
        for qi in range(tiles):
            if qi + 1 < tiles:
                scored(qi + 1)
            mixed(qi)
        return carry

    lax.fori_loop(0, groups, head, 0)
    dkey = unrotate(dk_scr[...].T * scale, cos_ref[...], sin_ref[...])
    qkv_ref[:, k_col:v_col] = pass_clip(dkey, qkv_ref[:, k_col:v_col])
    qkv_ref[:, v_col:v_col + HEAD_DIM] = pass_clip(dv_scr[...].T, qkv_ref[:, v_col:v_col + HEAD_DIM])
    gown_ref[...] = qkv_ref[own, :]
    gfar_ref[...] = qkv_ref[far, :]


def head_specs(half, slot, wide):
    table = held_whole(2 * half, HEAD_DIM)
    part = along_columns(half, wide)
    full = along_columns(half, slot)
    lse = along_columns(2 * half, wide)
    return table, part, full, lse


def attn_fwd(qkv_own, qkv_far, cos_t, sin_t, kv_loc):
    half = qkv_own.shape[0]
    slot = qkv_own.shape[1] // kv_loc
    groups = slot // HEAD_DIM - 2
    wide = groups * HEAD_DIM
    table, part, full, lse = head_specs(half, slot, wide)
    rows = jax.ShapeDtypeStruct((half, kv_loc * wide), jnp.bfloat16)
    return pl.pallas_call(
        functools.partial(attn_fwd_kernel, groups),
        grid=(kv_loc,),
        in_specs=[full, full, table, table],
        out_specs=[part, part, lse],
        out_shape=[rows, rows, jax.ShapeDtypeStruct((2 * half, kv_loc * wide), jnp.float32)],
        scratch_shapes=[pltpu.VMEM((2 * half, slot), jnp.bfloat16), pltpu.VMEM((2 * half, wide), jnp.bfloat16), pltpu.VMEM((2 * half, HEAD_DIM), jnp.bfloat16), pltpu.VMEM((HEAD_DIM, 2 * half), jnp.bfloat16), pltpu.VMEM((2, 2 * half, TILE_Q), jnp.float32), pltpu.VMEM((2, 2 * half, TILE_Q), jnp.bfloat16)],
        compiler_params=GRANT,
        cost_estimate=cost(12, 14),
        name="attn_fwd",
    )(qkv_own, qkv_far, cos_t, sin_t)


def attn_bwd(qkv_own, qkv_far, attn_own, attn_far, dattn_own, dattn_far, lse_t, cos_t, sin_t, kv_loc):
    half = qkv_own.shape[0]
    slot = qkv_own.shape[1] // kv_loc
    groups = slot // HEAD_DIM - 2
    wide = groups * HEAD_DIM
    table, part, full, lse = head_specs(half, slot, wide)
    return pl.pallas_call(
        functools.partial(attn_bwd_kernel, groups),
        grid=(kv_loc,),
        in_specs=[full, full, part, part, part, part, lse, table, table],
        out_specs=[full, full],
        out_shape=[jax.ShapeDtypeStruct(qkv_own.shape, jnp.bfloat16)] * 2,
        scratch_shapes=[pltpu.VMEM((2 * half, slot), jnp.bfloat16)] + [pltpu.VMEM((2 * half, wide), jnp.bfloat16)] * 2 + [pltpu.VMEM((2 * half, HEAD_DIM), jnp.bfloat16)] * 2 + [pltpu.VMEM((HEAD_DIM, 2 * half), jnp.float32)] * 2 + [pltpu.VMEM((2, TILE_Q, HEAD_DIM), jnp.bfloat16)] + [pltpu.VMEM((2, TILE_Q, 2 * half), jnp.bfloat16)] * 2,
        compiler_params=GRANT,
        cost_estimate=cost(25, 22),
        name="attn_bwd",
    )(qkv_own, qkv_far, attn_own, attn_far, dattn_own, dattn_far, lse_t, cos_t, sin_t)


def dw_qkv_kernel(n_rows, *refs):
    acts, grads, out_ref = refs[:n_rows], refs[n_rows:-1], refs[-1]
    slot = out_ref.shape[2]
    for n in range(out_ref.shape[1]):
        cols = slice(n * slot, (n + 1) * slot)
        acc = sum(dot(a[...], g[:, cols], TN) for a, g in zip(acts, grads))
        out_ref[:, n, :] = acc.astype(jnp.bfloat16)


def dw_qkv(acts, grads, kv_loc, tile=512):
    rows, d_model = acts[0].shape
    width = grads[0].shape[1]
    slot = width // kv_loc
    whole = held_whole(rows, width)
    part = along_columns(rows, tile)
    return pl.pallas_call(
        functools.partial(dw_qkv_kernel, len(acts)),
        grid=(d_model // tile,),
        in_specs=[part] * len(acts) + [whole] * len(grads),
        out_specs=pl.BlockSpec((tile, kv_loc, slot), lambda i: (i, 0, 0)),
        out_shape=jax.ShapeDtypeStruct((d_model, kv_loc, slot), jnp.bfloat16),
        compiler_params=GRANT,
        cost_estimate=cost(51, 60),
        name="dw_qkv",
    )(*acts, *grads)


def dw_out_kernel(n_rows, *refs):
    acts, grads, out_ref = refs[:n_rows], refs[n_rows:-1], refs[-1]
    out_ref[...] = sum(dot(a[...], g[...], TN) for a, g in zip(acts, grads)).astype(jnp.bfloat16)


def dw_out(acts, grads, tile=512):
    rows, width = acts[0].shape
    d_model = grads[0][1].shape[-1]
    whole = held_whole(rows, width)
    return pl.pallas_call(
        functools.partial(dw_out_kernel, len(acts)),
        grid=(d_model // tile,),
        in_specs=[whole] * len(acts) + [part_spec(g, b, (rows, tile), lambda i: (0, i)) for b, g in grads],
        out_specs=along_columns(width, tile),
        out_shape=jax.ShapeDtypeStruct((width, d_model), jnp.bfloat16),
        compiler_params=GRANT,
        cost_estimate=cost(39, 50),
        name="dw_out",
    )(*acts, *[g for _, g in grads])


def norm_fwd_kernel(x_ref, gain_ref, h_ref, stat_ref):
    def group(i, carry):
        rows = pl.ds(pl.multiple_of(i * 16, 16), 16)
        x_f32 = x_ref[0, rows, :].astype(jnp.float32)
        mean = jnp.mean(x_f32, axis=-1, keepdims=True)
        centered = x_f32 - mean
        rstd = lax.rsqrt(jnp.mean(centered * centered, axis=-1, keepdims=True) + LN_EPS)
        h_ref[rows, :] = (centered * rstd * gain_ref[...].astype(jnp.float32)[None, :]).astype(jnp.bfloat16)
        stat_ref[rows, :HEAD_DIM] = jnp.broadcast_to(mean, (16, HEAD_DIM))
        stat_ref[rows, HEAD_DIM:] = jnp.broadcast_to(rstd, (16, HEAD_DIM))
        return carry

    lax.fori_loop(0, x_ref.shape[1] // 16, group, 0, unroll=True)


def norm_fwd(x_seq, gain, b, tile=64):
    _, rows, d_model = x_seq.shape
    return pl.pallas_call(
        norm_fwd_kernel,
        grid=(rows // tile,),
        in_specs=[pl.BlockSpec((1, tile, d_model), lambda i: (b, i, 0)), pl.BlockSpec((d_model,), lambda i: (0,))],
        out_specs=[along_rows(tile, d_model), along_rows(tile, 2 * HEAD_DIM)],
        out_shape=[jax.ShapeDtypeStruct((rows, d_model), jnp.bfloat16), jax.ShapeDtypeStruct((rows, 2 * HEAD_DIM), jnp.float32)],
        compiler_params=GRANT,
        cost_estimate=cost(2, 7),
        name="norm_fwd",
    )(x_seq, gain)


def norm_split_kernel(x_ref, gain_ref, dy_ref, h_ref, stat_ref, dy0_ref, dy1_ref):
    norm_fwd_kernel(x_ref, gain_ref, h_ref, stat_ref)
    dy0_ref[...] = dy_ref[0]
    dy1_ref[...] = dy_ref[1]


def norm_split(x_seq, gain, y_grad, b, lead=64):
    _, rows, d_model = x_seq.shape
    row = along_rows(lead, d_model)
    return pl.pallas_call(
        norm_split_kernel,
        grid=(rows // lead,),
        in_specs=[pl.BlockSpec((1, lead, d_model), lambda i: (b, i, 0)), pl.BlockSpec((d_model,), lambda i: (0,)), pl.BlockSpec((2, lead, d_model), lambda i: (0, i, 0))],
        out_specs=[row, along_rows(lead, 2 * HEAD_DIM), row, row],
        out_shape=[jax.ShapeDtypeStruct((rows, d_model), jnp.bfloat16), jax.ShapeDtypeStruct((rows, 2 * HEAD_DIM), jnp.float32), jax.ShapeDtypeStruct((rows, d_model), jnp.bfloat16), jax.ShapeDtypeStruct((rows, d_model), jnp.bfloat16)],
        compiler_params=GRANT,
        cost_estimate=cost(2, 19),
        name="norm_split",
    )(x_seq, gain, y_grad)


def residual_kernel(split, x_ref, near0_ref, near1_ref, far0_ref, far1_ref, out_ref):
    def add(near, far):
        out_ref[0] = (x_ref[0].astype(jnp.float32) + (near[...] + far[...]).astype(jnp.float32)).astype(jnp.bfloat16)

    pl.when(pl.program_id(0) < split)(lambda: add(near0_ref, far0_ref))
    pl.when(pl.program_id(0) >= split)(lambda: add(near1_ref, far1_ref))


def residual_last_kernel(x_ref, near_ref, far_ref, held_ref, out_ref):
    out_ref[0] = (x_ref[0].astype(jnp.float32) + (near_ref[...] + far_ref[...]).astype(jnp.float32)).astype(jnp.bfloat16)


def norm_bwd_kernel(x_ref, dy_ref, gain_ref, near_ref, far_ref, stat_ref, *rest):
    dx_ref, dgain_ref, sum_ref = rest[-3:]

    @pl.when(pl.program_id(0) == 0)
    def _():
        sum_ref[...] = jnp.zeros_like(sum_ref)

    def group(i, carry):
        rows = pl.ds(pl.multiple_of(i * 16, 16), 16)
        mean, rstd = stat_ref[rows, :1], stat_ref[rows, HEAD_DIM:HEAD_DIM + 1]
        hat = (x_ref[0, rows, :].astype(jnp.float32) - mean) * rstd
        dh = (near_ref[rows, :] + far_ref[rows, :]).astype(jnp.float32)
        prod = dh * hat
        sum_ref[...] += prod[:8] + prod[8:]
        dhat = dh * gain_ref[...].astype(jnp.float32)[None, :]
        inner = dhat - jnp.mean(dhat, axis=-1, keepdims=True) - hat * jnp.mean(dhat * hat, axis=-1, keepdims=True)
        dx_ref[0, rows, :] = (dy_ref[0, rows, :].astype(jnp.float32) + inner * rstd).astype(jnp.bfloat16)
        return carry

    lax.fori_loop(0, x_ref.shape[1] // 16, group, 0, unroll=2)

    @pl.when(pl.program_id(0) == pl.num_programs(0) - 1)
    def _():
        dgain_ref[...] = jnp.sum(sum_ref[...], axis=0, keepdims=True)


def residual(x_seq, nears, fars, tile=64):
    _, rows, d_model = x_seq.shape
    split = rows // tile
    whole = pl.BlockSpec((1, tile, d_model), lambda i: (i // split, lax.rem(i, split), 0))
    first = pl.BlockSpec((tile, d_model), lambda i: (jnp.minimum(i, split - 1), 0))
    second = pl.BlockSpec((tile, d_model), lambda i: (jnp.maximum(i - split, 0), 0))
    return pl.pallas_call(
        functools.partial(residual_kernel, split),
        grid=(split + fars[1].shape[0] // tile,),
        in_specs=[whole, first, second, first, second],
        out_specs=whole,
        out_shape=jax.ShapeDtypeStruct(x_seq.shape, jnp.bfloat16),
        compiler_params=GRANT,
        cost_estimate=cost(4, 26),
        name="residual",
    )(x_seq, *nears, *fars)


def residual_last(x_seq, near, far, held, tile=32):
    _, rows, d_model = x_seq.shape
    base = (rows - far.shape[0]) // tile
    whole = pl.BlockSpec((1, tile, d_model), lambda i: (1, base + i, 0))
    return pl.pallas_call(
        residual_last_kernel,
        grid=(far.shape[0] // tile,),
        in_specs=[whole, pl.BlockSpec((tile, d_model), lambda i: (base + i, 0)), along_rows(tile, d_model), pl.BlockSpec(memory_space=pl.ANY)],
        out_specs=whole,
        out_shape=jax.ShapeDtypeStruct(x_seq.shape, jnp.bfloat16),
        input_output_aliases={3: 0},
        compiler_params=GRANT,
        cost_estimate=cost(1, 3),
        name="residual_last",
    )(x_seq, near, far, held)


def norm_bwd(x_seq, y_grad, gain, near, far, stat, b, base, held, tile=64):
    _, _, d_model = x_seq.shape
    first = base // tile
    whole = pl.BlockSpec((1, tile, d_model), lambda i: (b, first + i, 0))
    part = pl.BlockSpec((tile, d_model), lambda i: (first + i, 0))
    piece = along_rows(tile, d_model)
    row = held_whole(1, d_model)
    flat = pl.BlockSpec((d_model,), lambda i: (0,))
    keep = [] if held is None else [held]
    return pl.pallas_call(
        norm_bwd_kernel,
        grid=(far.shape[0] // tile,),
        in_specs=[whole, whole, flat, part, piece, pl.BlockSpec((tile, 2 * HEAD_DIM), lambda i: (first + i, 0))] + [pl.BlockSpec(memory_space=pl.ANY)] * len(keep),
        out_specs=[whole, row],
        out_shape=[jax.ShapeDtypeStruct(x_seq.shape, jnp.bfloat16), jax.ShapeDtypeStruct((1, d_model), jnp.float32)],
        input_output_aliases={6: 0} if keep else {},
        scratch_shapes=[pltpu.VMEM((8, d_model), jnp.float32)],
        compiler_params=GRANT,
        cost_estimate=cost(4, 16),
        name="norm_bwd",
    )(x_seq, y_grad, gain, near, far, stat, *keep)


def proj_deep_kernel(dims, a_ref, w_ref, out_ref, acc_ref):
    step, last = pl.program_id(0), pl.num_programs(0) - 1

    @pl.when(step == 0)
    def _():
        acc_ref[...] = jnp.zeros_like(acc_ref)

    acc_ref[...] += dot(a_ref[...], w_ref[...], dims)

    @pl.when(step == last)
    def _():
        out_ref[...] = acc_ref[...].astype(jnp.bfloat16)


def part_spec(a, b, block, index):
    if a.ndim == 2:
        return pl.BlockSpec(block, index)
    return pl.BlockSpec((None,) + block, lambda i: (b,) + index(i))


def proj_raw_kernel(n_parts, *refs):
    mine, theirs, w_ref = refs[:n_parts], refs[n_parts:2 * n_parts], refs[2 * n_parts]
    outs, flat_ref = refs[2 * n_parts + 1:3 * n_parts + 1], refs[3 * n_parts + 1]
    accs, joined = refs[3 * n_parts + 2:-1], refs[-1]
    step, last = pl.program_id(0), pl.num_programs(0) - 1
    core = lax.rem(lax.axis_index("tp"), 2)
    rows = mine[0].shape[0]

    @pl.when(step == 0)
    def _():
        for acc in accs:
            acc[...] = jnp.zeros_like(acc)

    flat_ref[...] = w_ref[...].reshape(flat_ref.shape)
    for b in range(n_parts):
        joined[b, pl.ds(pl.multiple_of(core * rows, rows), rows), :] = mine[b][...]
        joined[b, pl.ds(pl.multiple_of((1 - core) * rows, rows), rows), :] = theirs[b][...]
    for b, acc in enumerate(accs):
        acc[...] += dot(joined[b], flat_ref[...], NN)

    @pl.when(step == last)
    def _():
        for acc, out in zip(accs, outs):
            out[...] = acc[...].astype(jnp.bfloat16)


def proj_raw(mine, theirs, w, tile=512):
    rows, depth = mine[0].shape
    n_parts = len(mine)
    slots, slot = w.shape[1:]
    width = slots * slot
    return pl.pallas_call(
        functools.partial(proj_raw_kernel, n_parts),
        grid=(depth // tile,),
        in_specs=[along_columns(rows, tile)] * (2 * n_parts) + [pl.BlockSpec((tile, slots, slot), lambda i: (i, 0, 0))],
        out_specs=[held_whole(2 * rows, width)] * n_parts + [along_rows(tile, width)],
        out_shape=[jax.ShapeDtypeStruct((2 * rows, width), jnp.bfloat16)] * n_parts + [jax.ShapeDtypeStruct((depth, width), jnp.bfloat16)],
        scratch_shapes=[pltpu.VMEM((2 * rows, width), jnp.float32)] * n_parts + [pltpu.VMEM((n_parts, 2 * rows, tile), jnp.bfloat16)],
        compiler_params=GRANT,
        cost_estimate=matmul_cost(2 * n_parts * rows, depth, width),
        name="proj_raw",
    )(*mine, *theirs, w)


def proj_deep(a, w, dims, b=0, tile=1024):
    rows, depth = a.shape[-2:]
    width = w.shape[0] if dims is NT else w.shape[1]
    return pl.pallas_call(
        functools.partial(proj_deep_kernel, dims),
        grid=(depth // tile,),
        in_specs=[part_spec(a, b, (rows, tile), lambda i: (0, i)), along_columns(width, tile) if dims is NT else along_rows(tile, width)],
        out_specs=held_whole(rows, width),
        out_shape=jax.ShapeDtypeStruct((rows, width), jnp.bfloat16),
        scratch_shapes=[pltpu.VMEM((rows, width), jnp.float32)],
        compiler_params=GRANT,
        cost_estimate=matmul_cost(rows, depth, width),
        name="proj_deep",
    )(a, w)


def proj_wide_kernel(n_parts, dims, cut, *refs):
    w_ref, outs = refs[n_parts], refs[n_parts + 1:]
    first = dot(refs[0][...], w_ref[...], dims).astype(jnp.bfloat16)
    half, rest = first.shape[0] // 2, outs[1:]
    if cut == half:
        outs[0][...] = first
    else:
        rest = outs[2:]
        outs[0][:cut], outs[0][cut:] = first[:cut], first[half:half + cut]
        outs[1][:half - cut], outs[1][half - cut:] = first[cut:half], first[half + cut:]
    for a, out in zip(refs[1:n_parts], rest):
        out[...] = dot(a[...], w_ref[...], dims).astype(jnp.bfloat16)


def proj_wide(parts, w, dims, cut=None, tile=1024):
    rows, depth = parts[0].shape
    cut = cut or rows // 2
    width = w.shape[0] if dims is NT else w.shape[1]
    w_spec = along_rows(tile, depth) if dims is NT else along_columns(depth, tile)
    sizes = [2 * cut] + [rows - 2 * cut] * (2 * cut < rows) + [rows] * (len(parts) - 1)
    return pl.pallas_call(
        functools.partial(proj_wide_kernel, len(parts), dims, cut),
        grid=(width // tile,),
        in_specs=[held_whole(rows, depth)] * len(parts) + [w_spec],
        out_specs=[along_columns(size, tile) for size in sizes],
        out_shape=[jax.ShapeDtypeStruct((size, width), jnp.bfloat16) for size in sizes],
        compiler_params=GRANT,
        cost_estimate=matmul_cost(len(parts) * rows, depth, width),
        name="proj_wide",
    )(*parts, w)


def solution(mesh):
    n_tp = mesh.shape["tp"]
    pairs = [[i, i + 1] for i in range(0, n_tp, 2)]

    def swap(value, bit):
        return lax.ppermute(value, "tp", [(i, i ^ bit) for i in range(n_tp)])

    def pair_gather(value, axis=0):
        return lax.all_gather(value, "tp", axis_index_groups=pairs, axis=axis, tiled=True)

    def pair_scatter(value):
        return lax.psum_scatter(value, "tp", axis_index_groups=pairs, scatter_dimension=0, tiled=True)

    def staged_step(x_seq, ln_gain, w_qkv, w_out, y_grad):
        kv_loc = w_qkv.shape[1]
        gain = ln_gain
        token = [None]

        def run(fn, lead, *rest):
            if token[0] is not None:
                lead, _ = lax.optimization_barrier((lead, token[0]))
            result = fn(lead, *rest)
            token[0] = jax.tree.leaves(result)[0]
            return result

        h0, stat0 = run(lambda x: norm_fwd(x, gain, 0), x_seq)
        hx0 = swap(h0, 2)
        hs0 = swap(h0, 1)
        h1, stat1, dy0, dy1 = run(lambda x: norm_split(x, gain, y_grad, 1), x_seq)
        hs1 = swap(h1, 1)
        hx1 = swap(h1, 2)
        dyx0 = swap(dy0, 2)
        dyx1 = swap(dy1, 2)
        h_own0, h_own1 = pair_gather(h0), pair_gather(h1)
        dy_own = pair_gather(y_grad, 1)
        cos_t, sin_t = run(lambda p: lax.optimization_barrier(rope_tables(p)), jnp.arange(x_seq.shape[1] * n_tp, dtype=jnp.float32))
        qkv_own0, qkv_own1, w_flat = run(lambda h: proj_raw([h, h1], [hs0, hs1], w_qkv), h0)
        dattn_own0 = run(lambda d: proj_deep(d, w_out, NT, 0), dy_own)
        h_far0 = pair_gather(hx0)
        dattn_own1 = run(lambda d: proj_deep(d, w_out, NT, 1), dy_own)
        qkv_far0 = run(lambda h: proj_deep(h, w_flat, NN), h_far0)
        attn_own0, attn_far0, lse0 = run(lambda far: attn_fwd(qkv_own0, far, cos_t, sin_t, kv_loc), qkv_far0)
        h_far1 = pair_gather(hx1)
        o_far0, o_near0 = run(lambda a: proj_wide([a, attn_own0], w_out, NN), attn_far0)
        os_far0, os_near0 = pair_scatter(o_far0), pair_scatter(o_near0)
        qkv_far1 = run(lambda h: proj_deep(h, w_flat, NN), h_far1)
        ox0 = swap(os_far0, 2)
        attn_own1, attn_far1, lse1 = run(lambda far: attn_fwd(qkv_own1, far, cos_t, sin_t, kv_loc), qkv_far1)
        dy_far0 = pair_gather(dyx0)
        cut = x_seq.shape[1] * 3 // 4
        o_far1a, o_far1b, o_near1 = run(lambda a: proj_wide([a, attn_own1], w_out, NN, cut), attn_far1)
        os_far1a, os_far1b = pair_scatter(o_far1a), pair_scatter(o_far1b)
        os_near1 = pair_scatter(o_near1)
        dattn_far0 = run(lambda d: proj_deep(d, w_out, NT), dy_far0)
        ox1a, ox1b = swap(os_far1a, 2), swap(os_far1b, 2)
        dq_own0, dq_far0 = run(lambda d: attn_bwd(qkv_own0, qkv_far0, attn_own0, attn_far0, dattn_own0, d, lse0, cos_t, sin_t, kv_loc), dattn_far0)
        dy_far1 = pair_gather(dyx1)
        dh_far0, dh_near0 = run(lambda d: proj_wide([d, dq_own0], w_flat, NT), dq_far0)
        dhs_far0, dhs_near0 = pair_scatter(dh_far0), pair_scatter(dh_near0)
        dattn_far1 = run(lambda d: proj_deep(d, w_out, NT), dy_far1)
        dhx0 = swap(dhs_far0, 2)
        dq_own1, dq_far1 = run(lambda d: attn_bwd(qkv_own1, qkv_far1, attn_own1, attn_far1, dattn_own1, d, lse1, cos_t, sin_t, kv_loc), dattn_far1)
        dh_far1, dh_near1 = run(lambda d: proj_wide([d, dq_own1], w_flat, NT), dq_far1)
        dhs_far1, dhs_near1 = pair_scatter(dh_far1), pair_scatter(dh_near1)
        wout_grad = run(lambda a: dw_out([a, attn_far0, attn_own1, attn_far1], [(0, dy_own), (0, dy_far0), (1, dy_own), (0, dy_far1)]), attn_own0)
        dhx1 = swap(dhs_far1, 2)
        y_out = run(lambda near: residual(x_seq, [near, os_near1], [ox0, ox1a]), os_near0)
        wqkv_grad = run(lambda h: dw_qkv([h, h_far0, h_own1, h_far1], [dq_own0, dq_far0, dq_own1, dq_far1], kv_loc), h_own0)
        x_grad, gain0 = run(lambda near: norm_bwd(x_seq, y_grad, gain, near, dhx0, stat0, 0, 0, None), dhs_near0)
        x_grad, gain1 = run(lambda near: norm_bwd(x_seq, y_grad, gain, near, dhx1, stat1, 1, 0, x_grad), dhs_near1)
        y_out = run(lambda near: residual_last(x_seq, near, ox1b, y_out), os_near1)
        mine = gain0 + gain1
        gain_grad = (mine + swap(mine, 1) + swap(mine, 2) + swap(mine, 3)).astype(jnp.bfloat16)[0]
        return y_out, x_grad, gain_grad, wqkv_grad, wout_grad

    specs_in = (P('dp', 'tp', None), P(None), P(None, 'tp', None), P('tp', None), P('dp', 'tp', None))
    specs_out = (P('dp', 'tp', None), P('dp', 'tp', None), P('dp'), P('dp', 'tp', None), P(('dp', 'tp'), None))
    return jax.shard_map(staged_step, mesh=mesh, in_specs=specs_in, out_specs=specs_out, check_vma=False)
```
